32 devices in a mesh: seq: 16 (over z, y, x), chan: 2 (over core).
Axes of the slice: x: 2, y: 2, z: 4, core: 2. Of those that a mesh axis runs over, the one named last changes fastest.
Arguments:
- tokens: float32 [2048, 1024], P('seq', 'chan'), may hold values from -6 to 6
- gate_weight: float32 [1024, 1024], P(None, 'chan'), may hold values from -0.1875 to 0.1875
- value_weight: float32 [1024, 1024], P(None, 'chan'), may hold values from -0.1875 to 0.1875
- output_weight: float32 [1024, 1024], P('chan'), may hold values from -0.1875 to 0.1875
- wave_numbers: int32 [32], replicated, may hold values from 1 to 2047
- position_in: float32 [64, 64], replicated, may hold values from -0.75 to 0.75
- bias_in: float32 [64], replicated, may hold values from -3 to 3
- position_mid: float32 [64, 64], replicated, may hold values from -0.75 to 0.75
- bias_mid: float32 [64], replicated, may hold values from -3 to 3
- position_out: float32 [64, 1024], P(None, 'chan'), may hold values from -1 to 1
- decay_rate: float32 [1024], P('chan'), may hold values from 0.5 to 51.2
Outputs:
- mixed_tokens: float32 [2048, 1024], P('seq', 'chan')
The draws below stay inside these ranges and needn't reach their ends.
All inputs are finite; a program needn't handle non-finite values.
Results may differ from the reference program's by a relative error of at most 0.0003.
Values sent between devices are 32-bit elements; how exact they have to be, the bound alone decides.
A program may use at most 64 MiB of HBM per device.

```python
import math
import jax
import jax.numpy as jnp
from jax import lax

D = 1024
RPE_DIM = 64
PERIOD = 4096
L = 2048


def draw_tokens(key, part):
    key_a = jax.random.fold_in(jax.random.fold_in(key, 17), 0)
    return jax.random.truncated_normal(key_a, -6.0, 6.0, (L, D), jnp.float32)


def set_ends(array, stream_key, smallest, high):
    index_at = [jax.random.randint(jax.random.fold_in(stream_key, axis), (), 0, length) for axis, length in enumerate(array.shape)]
    longest = array.shape.index(max(array.shape))
    next_to = index_at[:longest] + [(index_at[longest] + 1) % array.shape[longest]] + index_at[longest + 1:]
    return array.at[tuple(index_at)].set(smallest).at[tuple(next_to)].set(high)


def block_scale(key, dims, shards, low, top_value):
    loudness = 1.0
    for axis_at, blocks in shards:
        draws = jax.random.uniform(jax.random.fold_in(jax.random.fold_in(key, 6), axis_at), (blocks,), jnp.float32, low / len(shards), top_value / len(shards))
        loudness = loudness * jnp.repeat(jnp.exp(draws), dims[axis_at] // blocks).reshape((-1,) + (1,) * (len(dims) - 1 - axis_at))
    return loudness


def centred(rng, extent, deviation, most, cuts=(), held_as=jnp.bfloat16):
    factor_of = block_scale(rng, extent, cuts, -0.22, 0.18) if cuts else 1.0
    drawn = jax.random.normal(rng, extent, jnp.float32) * deviation * factor_of
    return jnp.minimum(jnp.maximum(drawn, -most), most).astype(held_as)


def setup_inputs(seed: int = 0) -> dict:
    splits = jax.random.split(jax.random.key(seed), 12)
    return {
        "tokens": draw_tokens(jax.random.fold_in(splits[11], 71), 0),
        "gate_weight": centred(splits[1], (D, D), D ** -0.5, 0.1875, ((1, 2),), jnp.float32),
        "value_weight": centred(splits[2], (D, D), D ** -0.5, 0.1875, ((1, 2),), jnp.float32),
        "output_weight": centred(splits[3], (D, D), D ** -0.5, 0.1875, ((0, 2),), jnp.float32),
        "wave_numbers": set_ends(jax.random.randint(splits[4], (RPE_DIM // 2,), 1, PERIOD // 2), jax.random.fold_in(splits[4], 1), 1, (PERIOD // 2) - 1).astype(jnp.int32),
        "position_in": centred(splits[5], (RPE_DIM, RPE_DIM), RPE_DIM ** -0.5, 0.75, (), jnp.float32),
        "bias_in": centred(splits[6], (RPE_DIM,), 0.5, 3.0, (), jnp.float32),
        "position_mid": centred(splits[7], (RPE_DIM, RPE_DIM), RPE_DIM ** -0.5, 0.75, (), jnp.float32),
        "bias_mid": centred(splits[8], (RPE_DIM,), 0.5, 3.0, (), jnp.float32),
        "position_out": centred(splits[9], (RPE_DIM, D), (RPE_DIM // 2) ** -0.5, 1.0, ((1, 2),), jnp.float32),
        "decay_rate": jnp.clip(jnp.exp(math.log(51.2) - 4.6288867 * jax.random.uniform(splits[10], (D,), jnp.float32) ** block_scale(splits[10], (D,), ((0, 2),), -0.2, 0.2)), 0.5, 51.2),
    }


HIGHEST = lax.Precision.HIGHEST

def position_net(positions, wave_numbers, position_in, bias_in, position_mid, bias_mid, position_out, decay_rate, seq_length):
    phases = (positions % PERIOD)[:, None] * wave_numbers[None, :] % PERIOD
    angles = phases.astype(jnp.float32) * (2.0 * math.pi / PERIOD)
    features = jnp.concatenate([jnp.cos(angles), jnp.sin(angles)], axis=1)
    hidden = jax.nn.relu(jnp.dot(features, position_in, precision=HIGHEST) + bias_in)
    hidden = jax.nn.relu(jnp.dot(hidden, position_mid, precision=HIGHEST) + bias_mid)
    shapes = jnp.dot(hidden, position_out, precision=HIGHEST)
    spots = positions.astype(jnp.float32) / seq_length
    envelope = jnp.exp(-decay_rate[None, :] * spots[:, None]) * jnp.sqrt(2.0 * decay_rate / seq_length)[None, :]
    return shapes * envelope

def reference(tokens, gate_weight, value_weight, output_weight, wave_numbers, position_in, bias_in, position_mid, bias_mid, position_out, decay_rate):
    seq_length = tokens.shape[0]
    gated = jax.nn.silu(jnp.dot(tokens, gate_weight, precision=HIGHEST))
    values = jax.nn.silu(jnp.dot(tokens, value_weight, precision=HIGHEST))
    positions = jnp.arange(seq_length, dtype=jnp.int32)
    kernel = position_net(positions, wave_numbers, position_in, bias_in, position_mid, bias_mid, position_out, decay_rate, seq_length)
    padded_length = 2 * seq_length
    spectrum = jnp.fft.rfft(values, n=padded_length, axis=0) * jnp.fft.rfft(kernel, n=padded_length, axis=0)
    conv = jnp.fft.irfft(spectrum, n=padded_length, axis=0)[:seq_length]
    return jnp.dot(gated * conv, output_weight, precision=HIGHEST)
```

```python
import functools
import math

import jax
import jax.numpy as jnp
import numpy as np
from jax import lax
from jax.experimental import pallas as pl
from jax.experimental.pallas import tpu as pltpu
from jax.sharding import PartitionSpec as P

PERIOD = 4096
GROUPS = 2
F32 = jnp.float32
BF16 = jnp.bfloat16
MESH = pl.DeviceIdType.MESH


def split(a):
    hi = a.astype(BF16)
    return hi, (a - hi.astype(F32)).astype(BF16)


def mm(a, b, dims=((1,), (0,))):
    return lax.dot_general(a, b, (dims, ((), ())), preferred_element_type=F32)


def dot3(a, b, dims=((1,), (0,))):
    (ah, al), (bh, bl) = a, b
    return mm(ah, bh, dims) + (mm(ah, bl, dims) + mm(al, bh, dims))


def silu(v):
    return v / (1.0 + jnp.exp(-v))


def cmul_const(z, angle):
    c, s = math.cos(angle), math.sin(angle)
    re, im = z
    if abs(s) < 1e-12:
        return (re, im) if c > 0 else (-re, -im)
    if abs(c) < 1e-12:
        return (-im, re) if s > 0 else (im, -re)
    return (re * c - im * s, re * s + im * c)


def fft(xs, sign):
    n = len(xs)
    if n == 1:
        return xs
    even, odd = fft(xs[0::2], sign), fft(xs[1::2], sign)
    low, high = [], []
    for k in range(n // 2):
        er, ei = even[k]
        tr, ti = cmul_const(odd[k], sign * 2.0 * math.pi * k / n)
        low.append((er + tr, ei + ti))
        high.append((er - tr, ei - ti))
    return low + high


def tables(outer, inner):
    length = outer * inner
    r = np.arange(inner)
    turn = 2.0 * np.pi * np.outer(np.arange(outer) + 0.25, r) / length
    turns = np.concatenate([np.cos(turn), np.sin(turn)], 0).astype(np.float32)
    ang = 2.0 * np.pi * (np.outer(r, r) % inner) / inner
    c, s = np.cos(ang), np.sin(ang)
    fwd = np.block([[c, -s], [s, c]]).astype(np.float32)
    inv = (np.block([[c, s], [-s, c]]) / length).astype(np.float32)

    def halves(a):
        hi = a.astype(jnp.bfloat16)
        return [hi, (a - hi.astype(np.float32)).astype(jnp.bfloat16)]

    return turns, np.stack(halves(fwd) + halves(inv))


def column(row, first, count):
    n = row.shape[1]
    i = lax.broadcasted_iota(jnp.int32, (count, n), 0)
    j = lax.broadcasted_iota(jnp.int32, (count, n), 1)
    picked = jnp.where(j == i + first, jnp.broadcast_to(row, (count, n)), jnp.zeros_like(row))
    return jnp.sum(picked, axis=1, keepdims=True)


def forward(blocks, turn_ref, mat_ref):
    outer = len(blocks)
    step = -2.0 * math.pi / (4 * outer)
    twisted = [(b * math.cos(step * s), b * math.sin(step * s)) if s else (b, None) for s, b in enumerate(blocks)]
    twisted[0] = (blocks[0], jnp.zeros_like(blocks[0]))
    rows = []
    for k, (re, im) in enumerate(fft(twisted, -1.0)):
        c, s = turn_ref[k : k + 1, :], turn_ref[outer + k : outer + k + 1, :]
        rows.append(jnp.concatenate([re * c + im * s, im * c - re * s], axis=1))
    grid = jnp.concatenate(rows, axis=0)
    return dot3(split(grid), (mat_ref[0], mat_ref[1]))


def backward(spectrum, outer, turn_ref, mat_ref):
    back = dot3(split(spectrum), (mat_ref[2], mat_ref[3]))
    chans, inner = spectrum.shape[0] // outer, spectrum.shape[1] // 2
    zs = []
    for k in range(outer):
        re = back[k * chans : (k + 1) * chans, :inner]
        im = back[k * chans : (k + 1) * chans, inner:]
        c, s = turn_ref[k : k + 1, :], turn_ref[outer + k : outer + k + 1, :]
        zs.append((re * c - im * s, re * s + im * c))
    ys = fft(zs, 1.0)
    step = 2.0 * math.pi / (4 * outer)
    return [re * math.cos(step * s) - im * math.sin(step * s) for s, (re, im) in enumerate(ys)]


def position_blocks(outer, inner, chans, first, wave, w_in, b_in, w_mid, b_mid, w_out, decay):
    length = outer * inner
    waves = wave.shape[1]
    hid = w_in.shape[1]
    wcol = column(wave[...], 0, waves)
    unit = 2.0 * math.pi / PERIOD

    def trig(spots):
        ang = (lax.rem(spots * wcol, PERIOD)).astype(F32) * unit
        return jnp.cos(ang), jnp.sin(ang)

    rc, rs = trig(lax.broadcasted_iota(jnp.int32, (waves, inner), 1))
    sc, ss = trig(lax.broadcasted_iota(jnp.int32, (waves, max(outer, 128)), 1) * inner)
    bi, bm = column(b_in[...], 0, hid), column(b_mid[...], 0, w_mid.shape[1])
    wi, wm = split(w_in[...].T), split(w_mid[...].T)
    width = w_out.shape[1]
    i = lax.broadcasted_iota(jnp.int32, (chans, width), 0)
    j = lax.broadcasted_iota(jnp.int32, (chans, width), 1)
    pick = jnp.where(j == i + first, 1.0, 0.0).astype(BF16)
    oh, ol = split(w_out[...])
    nt = ((1,), (1,))
    own = (mm(pick, oh, nt).astype(BF16), mm(pick, ol, nt).astype(BF16))
    dec = column(decay[...], first, chans)
    gain = jnp.sqrt(2.0 * dec / length)
    per = max(1, 2048 // inner)
    blocks = []
    for s0 in range(0, outer, per):
        some = range(s0, min(outer, s0 + per))
        cs, sn = [], []
        for s in some:
            a, b = sc[:, s : s + 1], ss[:, s : s + 1]
            cs.append(rc * a - rs * b)
            sn.append(rs * a + rc * b)
        feats = jnp.concatenate([jnp.concatenate(cs, 1), jnp.concatenate(sn, 1)], 0)
        h = jnp.maximum(dot3(wi, split(feats)) + bi, 0.0)
        h = jnp.maximum(dot3(wm, split(h)) + bm, 0.0)
        shape = dot3(own, split(h))
        n = (lax.broadcasted_iota(jnp.int32, shape.shape, 1) + s0 * inner).astype(F32) / length
        kern = shape * (jnp.exp(-dec * n) * gain)
        blocks += [kern[:, q * inner : (q + 1) * inner] for q in range(len(some))]
    return blocks


def body(
    n, m, groups,
    tok_hbm, gate_hbm, value_hbm, out_hbm, turn_hbm, mat_hbm,
    wave_hbm, w_in_hbm, b_in_hbm, w_mid_hbm, b_mid_hbm, w_out_hbm, decay_hbm,
    result,
    wave, w_in, b_in, w_mid, b_mid, w_out, decay,
    tok, gate_w, value_w, out_w, turn, mat, sent, got, conv_out, conv_in, part_out, part_in,
    load_sem, up_sem, all_sem, tok_send, tok_recv, a_send, a_recv, b_send, b_recv, p_send, p_recv,
):
    me, mine = lax.axis_index("seq"), lax.axis_index("chan")
    rows, depth = tok_hbm.shape
    width = value_w.shape[1]
    chans = width // n
    per = chans // groups
    farthest = range(n - 1, 0, -1)

    def partner(i):
        if n & (n - 1):
            return lax.rem(me + i, n)
        bit, to = 1, 0
        while bit < n:
            here = lax.rem(me // bit, 2)
            to = to + (1 - here if i & bit else here) * bit
            bit *= 2
        return to


    barrier = pltpu.get_barrier_semaphore()
    for i in farthest:
        pl.semaphore_signal(barrier, inc=1, device_id={"seq": partner(i), "chan": 0}, device_id_type=MESH)

    @pl.when(mine == 0)
    def _():
        pl.semaphore_signal(barrier, inc=1, device_id={"chan": 1}, device_id_type=MESH)

    loads = [
        pltpu.make_async_copy(src, dst, load_sem.at[i])
        for i, (src, dst) in enumerate(
            [
                (tok_hbm, tok.at[mine]), (value_hbm, value_w), (gate_hbm, gate_w), (mat_hbm, mat), (turn_hbm, turn), (out_hbm, out_w),
                (wave_hbm, wave), (w_in_hbm, w_in), (b_in_hbm, b_in), (w_mid_hbm, w_mid), (b_mid_hbm, b_mid), (w_out_hbm, w_out), (decay_hbm, decay),
            ]
        )
    ]
    for c in loads:
        c.start()

    def arrived(ref, g, sem):
        block = ref.at[pl.ds(0, n - 1), pl.ds(g * per, per), :]
        pltpu.make_async_copy(block, block, sem).wait()

    def project(who, w_ref):
        lines = pl.ds(pl.multiple_of(who * depth, 8), depth)
        return dot3(split(tok[who]), split(w_ref[lines, :]))

    loads[0].wait()

    @pl.when(mine == 1)
    def _():
        pl.semaphore_wait(barrier, 1)
        pl.semaphore_signal(up_sem, inc=1, device_id={"chan": 0}, device_id_type=MESH)

    @pl.when(mine == 0)
    def _():
        pl.semaphore_wait(up_sem, 1)

    tok_copies = []
    for i in range(1, m):
        c = pltpu.make_async_remote_copy(
            src_ref=tok.at[mine], dst_ref=tok.at[mine], send_sem=tok_send.at[i], recv_sem=tok_recv.at[i],
            device_id={"chan": lax.rem(mine + i, m)}, device_id_type=MESH,
        )
        c.start()
        tok_copies.append(c)
    loads[1].wait()
    value_sum = project(mine, value_w)
    for i in range(1, m):
        tok_copies[i - 1].wait_recv()
        value_sum = value_sum + project(lax.rem(mine + m - i, m), value_w)
    sent[...] = silu(value_sum).T

    @pl.when(mine == 0)
    def _():
        pl.semaphore_wait(barrier, 2 * (n - 1))
        pl.semaphore_signal(all_sem, inc=1, device_id={"chan": 1}, device_id_type=MESH)

    @pl.when(mine == 1)
    def _():
        pl.semaphore_wait(all_sem, 1)

    for g in range(groups):
        for i in farthest:
            to = partner(i)
            c = pltpu.make_async_remote_copy(
                src_ref=sent.at[pl.ds(pl.multiple_of(to * chans + g * per, 8), per), :],
                dst_ref=got.at[me, pl.ds(g * per, per), :],
                send_sem=a_send, recv_sem=a_recv.at[g],
                device_id={"seq": to}, device_id_type=MESH,
            )
            c.start()
    got[me] = sent[pl.ds(pl.multiple_of(me * chans, 8), chans), :]

    for c in loads[3:5] + loads[6:]:
        c.wait()
    kernel_blocks = position_blocks(n, rows, chans, me * chans, wave, w_in, b_in, w_mid, b_mid, w_out, decay)
    kernel_specs = []
    for g in range(groups):
        kernel_specs.append(forward([b[g * per : (g + 1) * per] for b in kernel_blocks], turn, mat))

    for g in range(groups):
        arrived(got, g, a_recv.at[g])
        spec = forward([got[s, g * per : (g + 1) * per, :] for s in range(n)], turn, mat)
        vr, vi = spec[:, :rows], spec[:, rows:]
        kr, ki = kernel_specs[g][:, :rows], kernel_specs[g][:, rows:]
        prod = jnp.concatenate([vr * kr - vi * ki, vr * ki + vi * kr], axis=1)
        for s, y in enumerate(backward(prod, n, turn, mat)):
            conv_out[s, g * per : (g + 1) * per, :] = y
        for i in farthest:
            to = partner(i)
            c = pltpu.make_async_remote_copy(
                src_ref=conv_out.at[to, pl.ds(g * per, per), :],
                dst_ref=conv_in.at[me, pl.ds(g * per, per), :],
                send_sem=b_send, recv_sem=b_recv.at[g],
                device_id={"seq": to}, device_id_type=MESH,
            )
            c.start()
        conv_in[me, g * per : (g + 1) * per, :] = conv_out[me, g * per : (g + 1) * per, :]

    loads[2].wait()
    gate_sum = project(mine, gate_w)
    for i in range(1, m):
        gate_sum = gate_sum + project(lax.rem(mine + m - i, m), gate_w)
    gated = silu(gate_sum)
    loads[5].wait()
    gate_lines = gated.T.reshape(n, chans, rows)

    def partial(mixed, g, who):
        cols = pl.ds(pl.multiple_of(who * depth, 128), depth)
        lines = out_w[:, cols].reshape(n, chans, depth)[:, g * per : (g + 1) * per, :]
        return dot3(mixed, split(lines.reshape(n * per, depth)))

    sums = [0.0] * m
    for g in range(groups):
        some = slice(g * per, (g + 1) * per)
        arrived(conv_in, g, b_recv.at[g])
        mixed = split((gate_lines[:, some, :] * conv_in[:, some, :]).reshape(n * per, rows).T)
        if g < groups - 1:
            sums = [t + partial(mixed, g, lax.rem(mine + i, m)) for i, t in enumerate(sums)]

    p_copies = []
    for i in range(1, m):
        to = lax.rem(mine + i, m)
        part_out[i - 1] = sums[i] + partial(mixed, groups - 1, to)
        c = pltpu.make_async_remote_copy(
            src_ref=part_out.at[i - 1], dst_ref=part_in.at[i - 1], send_sem=p_send.at[i], recv_sem=p_recv.at[i],
            device_id={"chan": to}, device_id_type=MESH,
        )
        c.start()
        p_copies.append(c)
    total = sums[0] + partial(mixed, groups - 1, mine)
    for i in range(1, m):
        p_copies[i - 1].wait_recv()
        total = total + part_in[i - 1]
    result[...] = total
    for g in range(groups):
        arrived(got, g, a_send)
        arrived(conv_in, g, b_send)
    for c in tok_copies + p_copies:
        c.wait_send()


def on_device(
    tokens, gate_weight, value_weight, output_weight, wave_numbers,
    position_in, bias_in, position_mid, bias_mid, position_out, decay_rate,
):
    n, m = lax.axis_size("seq"), lax.axis_size("chan")
    rows, depth = tokens.shape
    width = gate_weight.shape[1]
    chans = width // n
    groups = max(1, min(GROUPS, chans // 8))
    assert m == 2
    turns, mats = tables(n, rows)
    hbm = pl.BlockSpec(memory_space=pl.ANY)
    vmem = pl.BlockSpec(memory_space=pltpu.VMEM)
    dma = pltpu.SemaphoreType.DMA
    return pl.pallas_call(
        functools.partial(body, n, m, groups),
        out_shape=pltpu.VMEM((rows, depth), F32),
        in_specs=[hbm] * 13,
        out_specs=vmem,
        scratch_shapes=[
            pltpu.VMEM((1, wave_numbers.shape[0]), jnp.int32),
            pltpu.VMEM(position_in.shape, F32),
            pltpu.VMEM((1, bias_in.shape[0]), F32),
            pltpu.VMEM(position_mid.shape, F32),
            pltpu.VMEM((1, bias_mid.shape[0]), F32),
            pltpu.VMEM(position_out.shape, F32),
            pltpu.VMEM((1, width), F32),
            pltpu.VMEM((m, rows, depth), F32),
            pltpu.VMEM(gate_weight.shape, F32),
            pltpu.VMEM(value_weight.shape, F32),
            pltpu.VMEM(output_weight.shape, F32),
            pltpu.VMEM(turns.shape, F32),
            pltpu.VMEM(mats.shape, BF16),
            pltpu.VMEM((width, rows), F32),
            pltpu.VMEM((n, chans, rows), F32),
            pltpu.VMEM((n, chans, rows), F32),
            pltpu.VMEM((n, chans, rows), F32),
            pltpu.VMEM((max(1, m - 1), rows, depth), F32),
            pltpu.VMEM((max(1, m - 1), rows, depth), F32),
            dma((13,)),
            pltpu.SemaphoreType.REGULAR,
            pltpu.SemaphoreType.REGULAR,
            dma((m,)), dma((m,)),
            dma, dma((groups,)),
            dma, dma((groups,)),
            dma((m,)), dma((m,)),
        ],
        compiler_params=pltpu.CompilerParams(collective_id=0, has_side_effects=True),
    )(
        tokens, gate_weight, value_weight, output_weight, jnp.asarray(turns), jnp.asarray(mats),
        wave_numbers[None, :], position_in, bias_in[None, :], position_mid, bias_mid[None, :],
        position_out, decay_rate[None, :],
    )


def solution(mesh):
    placed = (
        P("seq", "chan"), P(None, "chan"), P(None, "chan"), P("chan", None),
        P(), P(), P(), P(), P(), P(None, "chan"), P("chan"),
    )
    return jax.shard_map(
        on_device, mesh=mesh, in_specs=placed, out_specs=P("seq", "chan"), check_vma=False
    )
```

```python
import functools
import math

import jax
import jax.numpy as jnp
import numpy as np
from jax import lax
from jax.experimental import pallas as pl
from jax.experimental.pallas import tpu as pltpu
from jax.sharding import PartitionSpec as P

PERIOD = 4096
F32 = jnp.float32
BF16 = jnp.bfloat16
MESH = pl.DeviceIdType.MESH


def split(a):
    hi = a.astype(BF16)
    return hi, (a - hi.astype(F32)).astype(BF16)


def mm(a, b, dims=((1,), (0,))):
    return lax.dot_general(a, b, (dims, ((), ())), preferred_element_type=F32)


def dot3(a, b, dims=((1,), (0,))):
    (ah, al), (bh, bl) = a, b
    return mm(ah, bh, dims) + (mm(ah, bl, dims) + mm(al, bh, dims))


def silu(v):
    return v / (1.0 + jnp.exp(-v))


def cmul_const(z, angle):
    c, s = math.cos(angle), math.sin(angle)
    re, im = z
    if abs(s) < 1e-12:
        return (re, im) if c > 0 else (-re, -im)
    if abs(c) < 1e-12:
        return (-im, re) if s > 0 else (im, -re)
    return (re * c - im * s, re * s + im * c)


def fft(xs, sign):
    n = len(xs)
    if n == 1:
        return xs
    even, odd = fft(xs[0::2], sign), fft(xs[1::2], sign)
    low, high = [], []
    for k in range(n // 2):
        er, ei = even[k]
        tr, ti = cmul_const(odd[k], sign * 2.0 * math.pi * k / n)
        low.append((er + tr, ei + ti))
        high.append((er - tr, ei - ti))
    return low + high


def tables(outer, inner):
    length = outer * inner
    r = np.arange(inner)
    turn = 2.0 * np.pi * np.outer(np.arange(outer) + 0.25, r) / length
    turns = np.concatenate([np.cos(turn), np.sin(turn)], 0).astype(np.float32)
    ang = 2.0 * np.pi * (np.outer(r, r) % inner) / inner
    c, s = np.cos(ang), np.sin(ang)
    fwd = np.block([[c, -s], [s, c]]).astype(np.float32)
    inv = (np.block([[c, s], [-s, c]]) / length).astype(np.float32)

    def halves(a):
        hi = a.astype(jnp.bfloat16)
        return [hi, (a - hi.astype(np.float32)).astype(jnp.bfloat16)]

    return turns, np.stack(halves(fwd) + halves(inv))


def column(row, first, count):
    n = row.shape[1]
    i = lax.broadcasted_iota(jnp.int32, (count, n), 0)
    j = lax.broadcasted_iota(jnp.int32, (count, n), 1)
    picked = jnp.where(j == i + first, jnp.broadcast_to(row, (count, n)), jnp.zeros_like(row))
    return jnp.sum(picked, axis=1, keepdims=True)


def forward(blocks, turn_ref, mat_ref):
    outer = len(blocks)
    step = -2.0 * math.pi / (4 * outer)
    twisted = [(b * math.cos(step * s), b * math.sin(step * s)) if s else (b, None) for s, b in enumerate(blocks)]
    twisted[0] = (blocks[0], jnp.zeros_like(blocks[0]))
    rows = []
    for k, (re, im) in enumerate(fft(twisted, -1.0)):
        c, s = turn_ref[k : k + 1, :], turn_ref[outer + k : outer + k + 1, :]
        rows.append(jnp.concatenate([re * c + im * s, im * c - re * s], axis=1))
    grid = jnp.concatenate(rows, axis=0)
    return dot3(split(grid), (mat_ref[0], mat_ref[1]))


def backward(spectrum, outer, turn_ref, mat_ref):
    back = dot3(split(spectrum), (mat_ref[2], mat_ref[3]))
    chans, inner = spectrum.shape[0] // outer, spectrum.shape[1] // 2
    zs = []
    for k in range(outer):
        re = back[k * chans : (k + 1) * chans, :inner]
        im = back[k * chans : (k + 1) * chans, inner:]
        c, s = turn_ref[k : k + 1, :], turn_ref[outer + k : outer + k + 1, :]
        zs.append((re * c - im * s, re * s + im * c))
    ys = fft(zs, 1.0)
    step = 2.0 * math.pi / (4 * outer)
    return [re * math.cos(step * s) - im * math.sin(step * s) for s, (re, im) in enumerate(ys)]


def cmul(a, b):
    half = a.shape[1] // 2
    ar, ai, br, bi = a[:, :half], a[:, half:], b[:, :half], b[:, half:]
    return jnp.concatenate([ar * br - ai * bi, ar * bi + ai * br], axis=1)


def position_blocks(length, inner, parts, first, chans, wave, w_in, b_in, w_mid, b_mid, w_out, decay):
    waves = wave.shape[1]
    hid = w_in.shape[1]
    wcol = column(wave[...], 0, waves)
    unit = 2.0 * math.pi / PERIOD

    def trig(spots):
        ang = (lax.rem(spots * wcol, PERIOD)).astype(F32) * unit
        return jnp.cos(ang), jnp.sin(ang)

    rc, rs = trig(lax.broadcasted_iota(jnp.int32, (waves, inner), 1))
    sc, ss = trig(lax.broadcasted_iota(jnp.int32, (waves, max(length // inner, 128)), 1) * inner)
    bi, bm = column(b_in[...], 0, hid), column(b_mid[...], 0, w_mid.shape[1])
    wi, wm = split(w_in[...].T), split(w_mid[...].T)
    width = w_out.shape[1]
    oh, ol = split(w_out[...])
    nt = ((1,), (1,))
    i = lax.broadcasted_iota(jnp.int32, (chans, width), 0)
    j = lax.broadcasted_iota(jnp.int32, (chans, width), 1)
    pick = jnp.where(j == i + first, 1.0, 0.0).astype(BF16)
    own = (mm(pick, oh, nt).astype(BF16), mm(pick, ol, nt).astype(BF16))
    dec = column(decay[...], first, chans)
    gain = jnp.sqrt(2.0 * dec / length)
    most = max(1, 2048 // inner)
    result = []
    for start, stop in parts:
        blocks = []
        for s0 in range(start, stop, most):
            some = range(s0, min(stop, s0 + most))
            cs, sn = [], []
            for s in some:
                a, b = sc[:, s : s + 1], ss[:, s : s + 1]
                cs.append(rc * a - rs * b)
                sn.append(rs * a + rc * b)
            feats = jnp.concatenate([jnp.concatenate(cs, 1), jnp.concatenate(sn, 1)], 0)
            h = jnp.maximum(dot3(wi, split(feats)) + bi, 0.0)
            h = jnp.maximum(dot3(wm, split(h)) + bm, 0.0)
            shape = dot3(own, split(h))
            n = (lax.broadcasted_iota(jnp.int32, shape.shape, 1) + s0 * inner).astype(F32) / length
            kern = shape * (jnp.exp(-dec * n) * gain)
            blocks += [kern[:, q * inner : (q + 1) * inner] for q in range(len(some))]
        result.append(blocks)
    return result


def body(
    n, m, groups,
    tok_hbm, gate_hbm, value_hbm, out_hbm, turn_hbm, mat_hbm,
    wave_hbm, w_in_hbm, b_in_hbm, w_mid_hbm, b_mid_hbm, w_out_hbm, decay_hbm,
    result,
    wave, w_in, b_in, w_mid, b_mid, w_out, decay,
    tok, gate_w, value_w, out_w, turn, mat,
    sent, got, got_x, own_out, own_in, cross_out, cross_in, spec_ref, prod_ref, part_out, part_in,
    load_sem, up_sem, all_sem, tok_send, tok_recv,
    a_send, a_recv, x_send, x_recv, b_send, b_recv, y_send, y_recv, p_send, p_recv,
):
    me, mine = lax.axis_index("seq"), lax.axis_index("chan")
    rows, depth = tok_hbm.shape
    width = value_w.shape[1]
    half = n // 2
    side, idx = me // half, lax.rem(me, half)
    chans = width // half

    def flipped(at, i, count):
        if count & (count - 1):
            return lax.rem(at + i, count)
        bit, to = 1, 0
        while bit < count:
            here = lax.rem(at // bit, 2)
            to = to + (1 - here if i & bit else here) * bit
            bit *= 2
        return to

    barrier = pltpu.get_barrier_semaphore()
    lead = m - 1
    for i in range(n - 1, 0, -1):
        pl.semaphore_signal(barrier, inc=1, device_id={"seq": flipped(me, i, n), "chan": lead}, device_id_type=MESH)

    @pl.when(mine == lead)
    def _():
        pl.semaphore_signal(barrier, inc=1, device_id={"chan": 1 - lead}, device_id_type=MESH)

    loads = [
        pltpu.make_async_copy(src, dst, load_sem.at[i])
        for i, (src, dst) in enumerate(
            [
                (tok_hbm, tok.at[mine]), (value_hbm, value_w), (gate_hbm, gate_w), (mat_hbm, mat), (turn_hbm, turn), (out_hbm, out_w),
                (wave_hbm, wave), (w_in_hbm, w_in), (b_in_hbm, b_in), (w_mid_hbm, w_mid), (b_mid_hbm, b_mid), (w_out_hbm, w_out), (decay_hbm, decay),
            ]
        )
    ]
    for c in loads:
        c.start()

    def remote(src, dst, send, recv, to):
        c = pltpu.make_async_remote_copy(
            src_ref=src, dst_ref=dst, send_sem=send, recv_sem=recv, device_id=to, device_id_type=MESH
        )
        c.start()
        return c

    def drain(block, sem):
        pltpu.make_async_copy(block, block, sem).wait()

    def peers(ref, g):
        return ref.at[pl.ds(0, half - 1), pl.ds(groups[g][0], groups[g][1]), :]

    def lines(ref, who, g):
        first, count = groups[g]
        return ref.at[pl.ds(pl.multiple_of(who * chans + first, 8), count), :]

    def project(who, w_ref):
        where = pl.ds(pl.multiple_of(who * depth, 8), depth)
        return dot3(split(tok[who]), split(w_ref[where, :]))

    @pl.when(mine != lead)
    def _():
        pl.semaphore_wait(barrier, 1)
        pl.semaphore_signal(up_sem, inc=1, device_id={"chan": lead}, device_id_type=MESH)

    @pl.when(mine == lead)
    def _():
        pl.semaphore_wait(up_sem, 1)

    loads[0].wait()
    tok_copies = []
    for i in range(1, m):
        there = {"chan": lax.rem(mine + i, m)}
        tok_copies.append(remote(tok.at[mine], tok.at[mine], tok_send.at[i], tok_recv.at[i], there))
    loads[1].wait()
    value_sum = project(mine, value_w)
    for i in range(1, m):
        tok_copies[i - 1].wait_recv()
        value_sum = value_sum + project(lax.rem(mine + m - i, m), value_w)
    sent[...] = silu(value_sum).T

    @pl.when(mine == lead)
    def _():
        pl.semaphore_wait(barrier, m * (n - 1))
        pl.semaphore_signal(all_sem, inc=1, device_id={"chan": 1 - lead}, device_id_type=MESH)

    @pl.when(mine != lead)
    def _():
        pl.semaphore_wait(all_sem, 1)

    lower, by_value = side == 0, mine == lead
    near = sorted(range(half), key=lambda i: (bin(i % max(1, half // 2)).count("1"), i))

    @pl.when(jnp.logical_and(lower, by_value))
    def _():
        for g, (first, count) in enumerate(groups):
            for i in near:
                to = flipped(idx, i, half)
                there = got_x.at[idx, pl.ds(first, count), :]
                remote(lines(sent, to, g), there, x_send, x_recv.at[g], {"seq": half + to})

    for g, (first, count) in enumerate(groups):
        for i in range(half - 1, 0, -1):
            to = flipped(idx, i, half)
            there = got.at[idx, pl.ds(first, count), :]
            remote(lines(sent, to, g), there, a_send, a_recv.at[g], {"seq": side * half + to})
        got[idx, first : first + count, :] = lines(sent, idx, g)[...]

    for c in loads[3:5] + loads[6:]:
        c.wait()
    low, high = position_blocks(
        n * rows, rows, [(0, half), (half, n)], idx * chans, chans, wave, w_in, b_in, w_mid, b_mid, w_out, decay
    )
    kern, k_cross = [], []
    for first, count in groups:
        own = forward([b[first : first + count] for b in low], turn, mat)
        far = forward([b[first : first + count] for b in high], turn, mat)
        kern.append(own)
        k_cross.append(jnp.concatenate([far[:, :rows] - own[:, rows:], far[:, rows:] + own[:, :rows]], axis=1))

    def part(ref, g):
        first, count = groups[g]
        return [ref[s, first : first + count, :] for s in range(half)]

    for g, (first, count) in enumerate(groups):
        drain(peers(got, g), a_recv.at[g])
        spec = forward(part(got, g), turn, mat)
        spec_ref[g] = spec
        prod_ref[g] = cmul(spec, kern[g])

        @pl.when(jnp.logical_and(lower, jnp.logical_not(by_value)))
        def _():
            for s, y in enumerate(backward(cmul(spec_ref[g], k_cross[g]), half, turn, mat)):
                cross_out[s, first : first + count, :] = y
            for i in near:
                to = flipped(idx, i, half)
                here, there = cross_out.at[to, pl.ds(first, count), :], cross_in.at[idx, pl.ds(first, count), :]
                remote(here, there, y_send, y_recv.at[g], {"seq": half + to})

        @pl.when(jnp.logical_and(side == 1, by_value))
        def _():
            drain(got_x.at[:, pl.ds(first, count), :], x_recv.at[g])
            prod_ref[g] = prod_ref[g] + cmul(forward(part(got_x, g), turn, mat), k_cross[g])

        for s, y in enumerate(backward(prod_ref[g], half, turn, mat)):
            own_out[s, first : first + count, :] = y
        for i in range(half - 1, 0, -1):
            to = flipped(idx, i, half)
            here, there = own_out.at[to, pl.ds(first, count), :], own_in.at[idx, pl.ds(first, count), :]
            remote(here, there, b_send, b_recv.at[g], {"seq": side * half + to})
        own_in[idx, first : first + count, :] = own_out[idx, first : first + count, :]

    loads[2].wait()
    gate_sum = project(mine, gate_w)
    for i in range(1, m):
        gate_sum = gate_sum + project(lax.rem(mine + m - i, m), gate_w)
    gate_lines = silu(gate_sum).T.reshape(half, chans, rows)
    loads[5].wait()
    other = lax.rem(mine + 1, m)
    step = part_out.shape[2]

    def partial(mixed, g, start, size):
        first, count = groups[g]
        cols = pl.ds(pl.multiple_of(start, 128), size)
        some = out_w[:, cols].reshape(half, chans, size)[:, first : first + count, :]
        return dot3(mixed, split(some.reshape(half * count, size)))

    sums = [0.0, 0.0]
    for g, (first, count) in enumerate(groups):
        drain(peers(own_in, g), b_recv.at[g])

        @pl.when(jnp.logical_and(side == 1, jnp.logical_not(by_value)))
        def _():
            drain(cross_in.at[:, pl.ds(first, count), :], y_recv.at[g])
            own_in[:, first : first + count, :] = (
                own_in[:, first : first + count, :] + cross_in[:, first : first + count, :]
            )

        some = slice(first, first + count)
        mixed = split((gate_lines[:, some, :] * own_in[:, some, :]).reshape(half * count, rows).T)
        if g < len(groups) - 1:
            sums = [t + partial(mixed, g, who * depth, depth) for t, who in zip(sums, (mine, other))]

    for q in range(depth // step):
        ahead = sums[1][:, q * step : (q + 1) * step] if len(groups) > 1 else 0.0
        part_out[q] = ahead + partial(mixed, len(groups) - 1, other * depth + q * step, step)
        remote(part_out.at[q], part_in.at[q], p_send, p_recv, {"chan": other})
    total = sums[0] + partial(mixed, len(groups) - 1, mine * depth, depth)
    drain(part_in, p_recv)
    for q in range(depth // step):
        result[:, q * step : (q + 1) * step] = total[:, q * step : (q + 1) * step] + part_in[q]
    for g in range(len(groups)):
        drain(peers(got, g), a_send)
        drain(peers(own_in, g), b_send)

    @pl.when(jnp.logical_and(lower, by_value))
    def _():
        drain(got_x, x_send)

    @pl.when(jnp.logical_and(lower, jnp.logical_not(by_value)))
    def _():
        drain(cross_out, y_send)

    for c in tok_copies:
        c.wait_send()
    drain(part_out, p_send)


def on_device(
    tokens, gate_weight, value_weight, output_weight, wave_numbers,
    position_in, bias_in, position_mid, bias_mid, position_out, decay_rate,
):
    n, m = lax.axis_size("seq"), lax.axis_size("chan")
    rows, depth = tokens.shape
    width = gate_weight.shape[1]
    half = n // 2
    chans = width // half
    count = chans // 2 if chans % 16 == 0 else chans
    groups = [(first, count) for first in range(0, chans, count)]
    assert m == 2 and n % 2 == 0
    turns, mats = tables(half, rows)
    hbm = pl.BlockSpec(memory_space=pl.ANY)
    vmem = pl.BlockSpec(memory_space=pltpu.VMEM)
    dma = pltpu.SemaphoreType.DMA
    return pl.pallas_call(
        functools.partial(body, n, m, groups),
        out_shape=pltpu.VMEM((rows, depth), F32),
        in_specs=[hbm] * 13,
        out_specs=vmem,
        scratch_shapes=[
            pltpu.VMEM((1, wave_numbers.shape[0]), jnp.int32),
            pltpu.VMEM(position_in.shape, F32),
            pltpu.VMEM((1, bias_in.shape[0]), F32),
            pltpu.VMEM(position_mid.shape, F32),
            pltpu.VMEM((1, bias_mid.shape[0]), F32),
            pltpu.VMEM(position_out.shape, F32),
            pltpu.VMEM((1, width), F32),
            pltpu.VMEM((m, rows, depth), F32),
            pltpu.VMEM(gate_weight.shape, F32),
            pltpu.VMEM(value_weight.shape, F32),
            pltpu.VMEM(output_weight.shape, F32),
            pltpu.VMEM(turns.shape, F32),
            pltpu.VMEM(mats.shape, BF16),
            pltpu.VMEM((width, rows), F32),
            pltpu.VMEM((half, chans, rows), F32),
            pltpu.VMEM((half, chans, rows), F32),
            pltpu.VMEM((half, chans, rows), F32),
            pltpu.VMEM((half, chans, rows), F32),
            pltpu.VMEM((half, chans, rows), F32),
            pltpu.VMEM((half, chans, rows), F32),
            pltpu.VMEM((len(groups), half * count, 2 * rows), F32),
            pltpu.VMEM((len(groups), half * count, 2 * rows), F32),
            pltpu.VMEM((depth // 128, rows, 128), F32),
            pltpu.VMEM((depth // 128, rows, 128), F32),
            dma((13,)),
            pltpu.SemaphoreType.REGULAR,
            pltpu.SemaphoreType.REGULAR,
            dma((m,)), dma((m,)),
            dma, dma((len(groups),)), dma, dma((len(groups),)),
            dma, dma((len(groups),)), dma, dma((len(groups),)),
            dma, dma,
        ],
        compiler_params=pltpu.CompilerParams(collective_id=0, has_side_effects=True),
    )(
        tokens, gate_weight, value_weight, output_weight, jnp.asarray(turns), jnp.asarray(mats),
        wave_numbers[None, :], position_in, bias_in[None, :], position_mid, bias_mid[None, :],
        position_out, decay_rate[None, :],
    )


def solution(mesh):
    placed = (
        P("seq", "chan"), P(None, "chan"), P(None, "chan"), P("chan", None),
        P(), P(), P(), P(), P(), P(None, "chan"), P("chan"),
    )
    return jax.shard_map(
        on_device, mesh=mesh, in_specs=placed, out_specs=P("seq", "chan"), check_vma=False
    )
```

```python
import functools
import math

import jax
import jax.numpy as jnp
import numpy as np
from jax import lax
from jax.experimental import pallas as pl
from jax.experimental.pallas import tpu as pltpu
from jax.sharding import PartitionSpec as P

PERIOD = 4096
F32 = jnp.float32
BF16 = jnp.bfloat16
MESH = pl.DeviceIdType.MESH


def split(a):
    hi = a.astype(BF16)
    return hi, (a - hi.astype(F32)).astype(BF16)


def mm(a, b, dims=((1,), (0,))):
    return lax.dot_general(a, b, (dims, ((), ())), preferred_element_type=F32)


def dot3(a, b, dims=((1,), (0,))):
    (ah, al), (bh, bl) = a, b
    return mm(ah, bh, dims) + (mm(ah, bl, dims) + mm(al, bh, dims))


def silu(v):
    return v / (1.0 + jnp.exp(-v))


def cmul_const(z, angle):
    c, s = math.cos(angle), math.sin(angle)
    re, im = z
    if abs(s) < 1e-12:
        return (re, im) if c > 0 else (-re, -im)
    if abs(c) < 1e-12:
        return (-im, re) if s > 0 else (im, -re)
    return (re * c - im * s, re * s + im * c)


def fft(xs, sign):
    n = len(xs)
    if n == 1:
        return xs
    even, odd = fft(xs[0::2], sign), fft(xs[1::2], sign)
    low, high = [], []
    for k in range(n // 2):
        er, ei = even[k]
        tr, ti = cmul_const(odd[k], sign * 2.0 * math.pi * k / n)
        low.append((er + tr, ei + ti))
        high.append((er - tr, ei - ti))
    return low + high


def tables(outer, inner):
    length = outer * inner
    r = np.arange(inner)
    turn = 2.0 * np.pi * np.outer(np.arange(outer) + 0.25, r) / length
    turns = np.concatenate([np.cos(turn), np.sin(turn)], 0).astype(np.float32)
    ang = 2.0 * np.pi * (np.outer(r, r) % inner) / inner
    c, s = np.cos(ang), np.sin(ang)
    fwd = np.block([[c, -s], [s, c]]).astype(np.float32)
    inv = (np.block([[c, s], [-s, c]]) / length).astype(np.float32)

    def halves(a):
        hi = a.astype(jnp.bfloat16)
        return [hi, (a - hi.astype(np.float32)).astype(jnp.bfloat16)]

    return turns, np.stack(halves(fwd) + halves(inv))


def column(row, first, count):
    n = row.shape[1]
    i = lax.broadcasted_iota(jnp.int32, (count, n), 0)
    j = lax.broadcasted_iota(jnp.int32, (count, n), 1)
    picked = jnp.where(j == i + first, jnp.broadcast_to(row, (count, n)), jnp.zeros_like(row))
    return jnp.sum(picked, axis=1, keepdims=True)


def forward(blocks, turn_ref, mat_ref):
    outer = len(blocks)
    step = -2.0 * math.pi / (4 * outer)
    twisted = [(b * math.cos(step * s), b * math.sin(step * s)) if s else (b, None) for s, b in enumerate(blocks)]
    twisted[0] = (blocks[0], jnp.zeros_like(blocks[0]))
    rows = []
    for k, (re, im) in enumerate(fft(twisted, -1.0)):
        c, s = turn_ref[k : k + 1, :], turn_ref[outer + k : outer + k + 1, :]
        rows.append(jnp.concatenate([re * c + im * s, im * c - re * s], axis=1))
    grid = jnp.concatenate(rows, axis=0)
    return dot3(split(grid), (mat_ref[0], mat_ref[1]))


def backward(spectrum, outer, turn_ref, mat_ref):
    back = dot3(split(spectrum), (mat_ref[2], mat_ref[3]))
    chans, inner = spectrum.shape[0] // outer, spectrum.shape[1] // 2
    zs = []
    for k in range(outer):
        re = back[k * chans : (k + 1) * chans, :inner]
        im = back[k * chans : (k + 1) * chans, inner:]
        c, s = turn_ref[k : k + 1, :], turn_ref[outer + k : outer + k + 1, :]
        zs.append((re * c - im * s, re * s + im * c))
    ys = fft(zs, 1.0)
    step = 2.0 * math.pi / (4 * outer)
    return [re * math.cos(step * s) - im * math.sin(step * s) for s, (re, im) in enumerate(ys)]


def cmul(a, b):
    half = a.shape[1] // 2
    ar, ai, br, bi = a[:, :half], a[:, half:], b[:, :half], b[:, half:]
    return jnp.concatenate([ar * br - ai * bi, ar * bi + ai * br], axis=1)


def position_blocks(length, inner, parts, first, chans, wave, w_in, b_in, w_mid, b_mid, w_out, decay):
    waves = wave.shape[1]
    hid = w_in.shape[1]
    wcol = column(wave[...], 0, waves)
    unit = 2.0 * math.pi / PERIOD

    def trig(spots):
        ang = (lax.rem(spots * wcol, PERIOD)).astype(F32) * unit
        return jnp.cos(ang), jnp.sin(ang)

    rc, rs = trig(lax.broadcasted_iota(jnp.int32, (waves, inner), 1))
    sc, ss = trig(lax.broadcasted_iota(jnp.int32, (waves, max(length // inner, 128)), 1) * inner)
    bi, bm = column(b_in[...], 0, hid), column(b_mid[...], 0, w_mid.shape[1])
    wi, wm = split(w_in[...].T), split(w_mid[...].T)
    width = w_out.shape[1]
    oh, ol = split(w_out[...])
    nt = ((1,), (1,))
    i = lax.broadcasted_iota(jnp.int32, (chans, width), 0)
    j = lax.broadcasted_iota(jnp.int32, (chans, width), 1)
    pick = jnp.where(j == i + first, 1.0, 0.0).astype(BF16)
    own = (mm(pick, oh, nt).astype(BF16), mm(pick, ol, nt).astype(BF16))
    dec = column(decay[...], first, chans)
    gain = jnp.sqrt(2.0 * dec / length)
    most = max(1, 2048 // inner)
    result = []
    for start, stop in parts:
        blocks = []
        for s0 in range(start, stop, most):
            some = range(s0, min(stop, s0 + most))
            cs, sn = [], []
            for s in some:
                a, b = sc[:, s : s + 1], ss[:, s : s + 1]
                cs.append(rc * a - rs * b)
                sn.append(rs * a + rc * b)
            feats = jnp.concatenate([jnp.concatenate(cs, 1), jnp.concatenate(sn, 1)], 0)
            h = jnp.maximum(dot3(wi, split(feats)) + bi, 0.0)
            h = jnp.maximum(dot3(wm, split(h)) + bm, 0.0)
            shape = dot3(own, split(h))
            n = (lax.broadcasted_iota(jnp.int32, shape.shape, 1) + s0 * inner).astype(F32) / length
            kern = shape * (jnp.exp(-dec * n) * gain)
            blocks += [kern[:, q * inner : (q + 1) * inner] for q in range(len(some))]
        result.append(blocks)
    return result


def body(
    n, m, groups,
    tok_hbm, gate_hbm, value_hbm, out_hbm, turn_hbm, mat_hbm,
    wave_hbm, w_in_hbm, b_in_hbm, w_mid_hbm, b_mid_hbm, w_out_hbm, decay_hbm,
    result,
    wave, w_in, b_in, w_mid, b_mid, w_out, decay,
    tok, gate_w, value_w, out_w, turn, mat,
    sent, got, got_x, own_out, own_in, cross_out, cross_in, spec_ref, prod_ref, w_high, w_low, part_out, part_in,
    load_sem, up_sem, all_sem, far_sem, tok_send, tok_recv,
    a_send, a_recv, x_send, x_recv, b_send, b_recv, y_send, y_recv, p_send, p_recv,
):
    me, mine = lax.axis_index("seq"), lax.axis_index("chan")
    rows, depth = tok_hbm.shape
    width = value_w.shape[1]
    half = n // 2
    side, idx = me // half, lax.rem(me, half)
    chans = width // half

    def flipped(at, i, count):
        if count & (count - 1):
            return lax.rem(at + i, count)
        bit, to = 1, 0
        while bit < count:
            here = lax.rem(at // bit, 2)
            to = to + (1 - here if i & bit else here) * bit
            bit *= 2
        return to

    barrier = pltpu.get_barrier_semaphore()
    lead, quarter = m - 1, half // 2
    lower, by_value = side == 0, mine == lead
    first_z, second_z = jnp.logical_and(lower, idx < quarter), jnp.logical_and(lower, idx >= quarter)
    by_result = jnp.logical_not(by_value)
    for i in range(half - 1, 0, -1):
        to = side * half + flipped(idx, i, half)
        pl.semaphore_signal(barrier, inc=1, device_id={"seq": to, "chan": lead}, device_id_type=MESH)

    @pl.when(jnp.logical_not(lower))
    def _():
        for to in range(quarter, half):
            pl.semaphore_signal(barrier, inc=1, device_id={"seq": to, "chan": lead}, device_id_type=MESH)

    @pl.when(mine == lead)
    def _():
        pl.semaphore_signal(barrier, inc=1, device_id={"chan": 1 - lead}, device_id_type=MESH)

    loads = [
        pltpu.make_async_copy(src, dst, load_sem.at[i])
        for i, (src, dst) in enumerate(
            [
                (tok_hbm, tok.at[mine]), (value_hbm, value_w), (gate_hbm, gate_w), (mat_hbm, mat), (turn_hbm, turn), (out_hbm, out_w),
                (wave_hbm, wave), (w_in_hbm, w_in), (b_in_hbm, b_in), (w_mid_hbm, w_mid), (b_mid_hbm, b_mid), (w_out_hbm, w_out), (decay_hbm, decay),
            ]
        )
    ]
    for c in loads:
        c.start()

    def remote(src, dst, send, recv, to):
        c = pltpu.make_async_remote_copy(
            src_ref=src, dst_ref=dst, send_sem=send, recv_sem=recv, device_id=to, device_id_type=MESH
        )
        c.start()
        return c

    def drain(block, sem):
        pltpu.make_async_copy(block, block, sem).wait()

    def peers(ref, g):
        return ref.at[pl.ds(0, half - 1), pl.ds(groups[g][0], groups[g][1]), :]

    def lines(ref, who, g):
        first, count = groups[g]
        return ref.at[pl.ds(pl.multiple_of(who * chans + first, 8), count), :]

    def weight(who, w_ref):
        return split(w_ref[pl.ds(pl.multiple_of(who * depth, 8), depth), :])

    def project(who, w_ref):
        return dot3(split(tok[who]), weight(who, w_ref))

    @pl.when(mine != lead)
    def _():
        pl.semaphore_wait(barrier, 1)
        pl.semaphore_signal(up_sem, inc=1, device_id={"chan": lead}, device_id_type=MESH)

    @pl.when(mine == lead)
    def _():
        pl.semaphore_wait(up_sem, 1)

    loads[0].wait()
    tok_copies = []
    for i in range(1, m):
        there = {"chan": lax.rem(mine + i, m)}
        tok_copies.append(remote(tok.at[mine], tok.at[mine], tok_send.at[i], tok_recv.at[i], there))
    loads[1].wait()
    value_sum = project(mine, value_w)
    ahead = weight(1 - mine, value_w)
    tok_copies[0].wait_recv()
    value_sum = value_sum + dot3(split(tok[1 - mine]), ahead)
    sent[...] = silu(value_sum).T

    near = sorted(range(half), key=lambda i: (bin(i % max(1, half // 2)).count("1"), i))

    def tell(sem, **who):
        pl.semaphore_signal(sem, inc=1, device_id=who, device_id_type=MESH)

    def cross_values():
        for g, (first, count) in enumerate(groups):
            for i in near:
                to = flipped(idx, i, half)
                there = got_x.at[idx, pl.ds(first, count), :]
                remote(lines(sent, to, g), there, x_send, x_recv.at[g], {"seq": half + to})

    @pl.when(jnp.logical_and(by_value, jnp.logical_not(second_z)))
    def _():
        pl.semaphore_wait(barrier, m * (half - 1))
        tell(all_sem, chan=1 - lead)

        @pl.when(jnp.logical_and(lower, idx + quarter < half))
        def _():
            tell(all_sem, seq=idx + quarter, chan=1 - lead)

    @pl.when(jnp.logical_and(by_value, second_z))
    def _():
        pl.semaphore_wait(barrier, m * (n - 1))
        tell(far_sem, chan=1 - lead)

        @pl.when(idx >= quarter)
        def _():
            tell(far_sem, seq=idx - quarter)

        cross_values()

    @pl.when(by_result)
    def _():
        pl.semaphore_wait(all_sem, 1)

    for g, (first, count) in enumerate(groups):
        for i in range(half - 1, 0, -1):
            to = flipped(idx, i, half)
            there = got.at[idx, pl.ds(first, count), :]
            remote(lines(sent, to, g), there, a_send, a_recv.at[g], {"seq": side * half + to})
        got[idx, first : first + count, :] = lines(sent, idx, g)[...]

    @pl.when(jnp.logical_and(by_value, first_z))
    def _():
        pl.semaphore_wait(far_sem, 1)
        tell(far_sem, chan=1 - lead)
        cross_values()

    for c in loads[3:5] + loads[6:]:
        c.wait()
    low, high = position_blocks(
        n * rows, rows, [(0, half), (half, n)], idx * chans, chans, wave, w_in, b_in, w_mid, b_mid, w_out, decay
    )
    kern, k_cross = [], []
    for first, count in groups:
        own = forward([b[first : first + count] for b in low], turn, mat)
        far = forward([b[first : first + count] for b in high], turn, mat)
        kern.append(own)
        k_cross.append(jnp.concatenate([far[:, :rows] - own[:, rows:], far[:, rows:] + own[:, :rows]], axis=1))

    def part(ref, g):
        first, count = groups[g]
        return [ref[s, first : first + count, :] for s in range(half)]

    for g, (first, count) in enumerate(groups):
        drain(peers(got, g), a_recv.at[g])
        spec = forward(part(got, g), turn, mat)
        spec_ref[g] = spec
        prod_ref[g] = cmul(spec, kern[g])

        @pl.when(jnp.logical_and(side == 1, by_value))
        def _():
            drain(got_x.at[:, pl.ds(first, count), :], x_recv.at[g])
            prod_ref[g] = prod_ref[g] + cmul(forward(part(got_x, g), turn, mat), k_cross[g])

        for s, y in enumerate(backward(prod_ref[g], half, turn, mat)):
            own_out[s, first : first + count, :] = y
        for i in range(half - 1, 0, -1):
            to = flipped(idx, i, half)
            here, there = own_out.at[to, pl.ds(first, count), :], own_in.at[idx, pl.ds(first, count), :]
            remote(here, there, b_send, b_recv.at[g], {"seq": side * half + to})
        own_in[idx, first : first + count, :] = own_out[idx, first : first + count, :]

        @pl.when(jnp.logical_and(lower, by_result))
        def _():
            for s, y in enumerate(backward(cmul(spec_ref[g], k_cross[g]), half, turn, mat)):
                cross_out[s, first : first + count, :] = y
            if g == 0:
                pl.semaphore_wait(far_sem, 1)
            for i in near:
                to = flipped(idx, i, half)
                here, there = cross_out.at[to, pl.ds(first, count), :], cross_in.at[idx, pl.ds(first, count), :]
                remote(here, there, y_send, y_recv.at[g], {"seq": half + to})

    loads[2].wait()
    gate_sum = project(mine, gate_w)
    for i in range(1, m):
        gate_sum = gate_sum + project(lax.rem(mine + m - i, m), gate_w)
    gate_lines = silu(gate_sum).T.reshape(half, chans, rows)
    loads[5].wait()
    for g, (first, count) in enumerate(groups):
        some = out_w[...].reshape(half, chans, m * depth)[:, first : first + count, :]
        w_high[g], w_low[g] = split(some.reshape(half * count, m * depth))
    other = lax.rem(mine + 1, m)

    def partial(mixed, g, start, size):
        cols = pl.ds(pl.multiple_of(start, 128), size)
        return dot3(mixed, (w_high[g, :, cols], w_low[g, :, cols]))

    sums = [0.0, 0.0]
    for g, (first, count) in enumerate(groups):
        drain(peers(own_in, g), b_recv.at[g])

        @pl.when(jnp.logical_and(side == 1, by_result))
        def _():
            drain(cross_in.at[:, pl.ds(first, count), :], y_recv.at[g])
            own_in[:, first : first + count, :] = (
                own_in[:, first : first + count, :] + cross_in[:, first : first + count, :]
            )

        some = slice(first, first + count)
        mixed = split((gate_lines[:, some, :] * own_in[:, some, :]).reshape(half * count, rows).T)
        if g < len(groups) - 1:
            sums = [t + partial(mixed, g, who * depth, depth) for t, who in zip(sums, (mine, other))]

    part_out[...] = sums[1] + partial(mixed, len(groups) - 1, other * depth, depth)
    remote(part_out, part_in, p_send, p_recv, {"chan": other})
    total = sums[0] + partial(mixed, len(groups) - 1, mine * depth, depth)
    drain(part_in, p_recv)
    result[...] = total + part_in[...]
    for g in range(len(groups)):
        drain(peers(got, g), a_send)
        drain(peers(own_in, g), b_send)

    @pl.when(jnp.logical_and(lower, by_value))
    def _():
        drain(got_x, x_send)

    @pl.when(jnp.logical_and(lower, by_result))
    def _():
        drain(cross_out, y_send)

    for c in tok_copies:
        c.wait_send()
    drain(part_out, p_send)


def on_device(
    tokens, gate_weight, value_weight, output_weight, wave_numbers,
    position_in, bias_in, position_mid, bias_mid, position_out, decay_rate,
):
    n, m = lax.axis_size("seq"), lax.axis_size("chan")
    rows, depth = tokens.shape
    width = gate_weight.shape[1]
    half = n // 2
    chans = width // half
    count = chans // 2 if chans % 16 == 0 else chans
    groups = [(first, count) for first in range(0, chans, count)]
    assert m == 2 and n % 2 == 0
    turns, mats = tables(half, rows)
    hbm = pl.BlockSpec(memory_space=pl.ANY)
    vmem = pl.BlockSpec(memory_space=pltpu.VMEM)
    dma = pltpu.SemaphoreType.DMA
    return pl.pallas_call(
        functools.partial(body, n, m, groups),
        out_shape=pltpu.VMEM((rows, depth), F32),
        in_specs=[hbm] * 13,
        out_specs=vmem,
        scratch_shapes=[
            pltpu.VMEM((1, wave_numbers.shape[0]), jnp.int32),
            pltpu.VMEM(position_in.shape, F32),
            pltpu.VMEM((1, bias_in.shape[0]), F32),
            pltpu.VMEM(position_mid.shape, F32),
            pltpu.VMEM((1, bias_mid.shape[0]), F32),
            pltpu.VMEM(position_out.shape, F32),
            pltpu.VMEM((1, width), F32),
            pltpu.VMEM((m, rows, depth), F32),
            pltpu.VMEM(gate_weight.shape, F32),
            pltpu.VMEM(value_weight.shape, F32),
            pltpu.VMEM(output_weight.shape, F32),
            pltpu.VMEM(turns.shape, F32),
            pltpu.VMEM(mats.shape, BF16),
            pltpu.VMEM((width, rows), F32),
            pltpu.VMEM((half, chans, rows), F32),
            pltpu.VMEM((half, chans, rows), F32),
            pltpu.VMEM((half, chans, rows), F32),
            pltpu.VMEM((half, chans, rows), F32),
            pltpu.VMEM((half, chans, rows), F32),
            pltpu.VMEM((half, chans, rows), F32),
            pltpu.VMEM((len(groups), half * count, 2 * rows), F32),
            pltpu.VMEM((len(groups), half * count, 2 * rows), F32),
            pltpu.VMEM((len(groups), half * count, m * depth), BF16),
            pltpu.VMEM((len(groups), half * count, m * depth), BF16),
            pltpu.VMEM((rows, depth), F32),
            pltpu.VMEM((rows, depth), F32),
            dma((13,)),
            pltpu.SemaphoreType.REGULAR,
            pltpu.SemaphoreType.REGULAR,
            pltpu.SemaphoreType.REGULAR,
            dma((m,)), dma((m,)),
            dma, dma((len(groups),)), dma, dma((len(groups),)),
            dma, dma((len(groups),)), dma, dma((len(groups),)),
            dma, dma,
        ],
        compiler_params=pltpu.CompilerParams(collective_id=0, has_side_effects=True),
    )(
        tokens, gate_weight, value_weight, output_weight, jnp.asarray(turns), jnp.asarray(mats),
        wave_numbers[None, :], position_in, bias_in[None, :], position_mid, bias_mid[None, :],
        position_out, decay_rate[None, :],
    )


def solution(mesh):
    placed = (
        P("seq", "chan"), P(None, "chan"), P(None, "chan"), P("chan", None),
        P(), P(), P(), P(), P(), P(None, "chan"), P("chan"),
    )
    return jax.shard_map(
        on_device, mesh=mesh, in_specs=placed, out_specs=P("seq", "chan"), check_vma=False
    )
```

```python
import functools
import math

import jax
import jax.numpy as jnp
import numpy as np
from jax import lax
from jax.experimental import pallas as pl
from jax.experimental.pallas import tpu as pltpu
from jax.sharding import PartitionSpec as P

PERIOD = 4096
F32 = jnp.float32
BF16 = jnp.bfloat16
MESH = pl.DeviceIdType.MESH


def split(a):
    hi = a.astype(BF16)
    return hi, (a - hi.astype(F32)).astype(BF16)


def mm(a, b, dims=((1,), (0,))):
    return lax.dot_general(a, b, (dims, ((), ())), preferred_element_type=F32)


def dot3(a, b, dims=((1,), (0,))):
    (ah, al), (bh, bl) = a, b
    return mm(ah, bh, dims) + (mm(ah, bl, dims) + mm(al, bh, dims))


def silu(v):
    return v / (1.0 + jnp.exp(-v))


def cmul_const(z, angle):
    c, s = math.cos(angle), math.sin(angle)
    re, im = z
    if abs(s) < 1e-12:
        return (re, im) if c > 0 else (-re, -im)
    if abs(c) < 1e-12:
        return (-im, re) if s > 0 else (im, -re)
    return (re * c - im * s, re * s + im * c)


def fft(xs, sign):
    n = len(xs)
    if n == 1:
        return xs
    even, odd = fft(xs[0::2], sign), fft(xs[1::2], sign)
    low, high = [], []
    for k in range(n // 2):
        er, ei = even[k]
        tr, ti = cmul_const(odd[k], sign * 2.0 * math.pi * k / n)
        low.append((er + tr, ei + ti))
        high.append((er - tr, ei - ti))
    return low + high


def tables(outer, inner):
    length = outer * inner
    r = np.arange(inner)
    turn = 2.0 * np.pi * np.outer(np.arange(outer) + 0.25, r) / length
    turns = np.concatenate([np.cos(turn), np.sin(turn)], 0).astype(np.float32)
    ang = 2.0 * np.pi * (np.outer(r, r) % inner) / inner
    c, s = np.cos(ang), np.sin(ang)
    fwd = np.block([[c, -s], [s, c]]).astype(np.float32)
    inv = (np.block([[c, s], [-s, c]]) / length).astype(np.float32)

    def halves(a):
        hi = a.astype(jnp.bfloat16)
        return [hi, (a - hi.astype(np.float32)).astype(jnp.bfloat16)]

    return turns, np.stack(halves(fwd) + halves(inv))


def column(row, first, count):
    n = row.shape[1]
    i = lax.broadcasted_iota(jnp.int32, (count, n), 0)
    j = lax.broadcasted_iota(jnp.int32, (count, n), 1)
    picked = jnp.where(j == i + first, jnp.broadcast_to(row, (count, n)), jnp.zeros_like(row))
    return jnp.sum(picked, axis=1, keepdims=True)


def forward(blocks, turn_ref, mat_ref):
    outer = len(blocks)
    step = -2.0 * math.pi / (4 * outer)
    twisted = [(b * math.cos(step * s), b * math.sin(step * s)) if s else (b, None) for s, b in enumerate(blocks)]
    twisted[0] = (blocks[0], jnp.zeros_like(blocks[0]))
    rows = []
    for k, (re, im) in enumerate(fft(twisted, -1.0)):
        c, s = turn_ref[k : k + 1, :], turn_ref[outer + k : outer + k + 1, :]
        rows.append(jnp.concatenate([re * c + im * s, im * c - re * s], axis=1))
    grid = jnp.concatenate(rows, axis=0)
    return dot3(split(grid), (mat_ref[0], mat_ref[1]))


def backward(spectrum, outer, turn_ref, mat_ref):
    back = dot3(split(spectrum), (mat_ref[2], mat_ref[3]))
    chans, inner = spectrum.shape[0] // outer, spectrum.shape[1] // 2
    zs = []
    for k in range(outer):
        re = back[k * chans : (k + 1) * chans, :inner]
        im = back[k * chans : (k + 1) * chans, inner:]
        c, s = turn_ref[k : k + 1, :], turn_ref[outer + k : outer + k + 1, :]
        zs.append((re * c - im * s, re * s + im * c))
    ys = fft(zs, 1.0)
    step = 2.0 * math.pi / (4 * outer)
    return [re * math.cos(step * s) - im * math.sin(step * s) for s, (re, im) in enumerate(ys)]


def cmul(a, b):
    half = a.shape[1] // 2
    ar, ai, br, bi = a[:, :half], a[:, half:], b[:, :half], b[:, half:]
    return jnp.concatenate([ar * br - ai * bi, ar * bi + ai * br], axis=1)


def position_blocks(length, inner, parts, first, chans, wave, w_in, b_in, w_mid, b_mid, w_out, decay):
    waves = wave.shape[1]
    hid = w_in.shape[1]
    wcol = column(wave[...], 0, waves)
    unit = 2.0 * math.pi / PERIOD

    def trig(spots):
        ang = (lax.rem(spots * wcol, PERIOD)).astype(F32) * unit
        return jnp.cos(ang), jnp.sin(ang)

    rc, rs = trig(lax.broadcasted_iota(jnp.int32, (waves, inner), 1))
    sc, ss = trig(lax.broadcasted_iota(jnp.int32, (waves, max(length // inner, 128)), 1) * inner)
    bi, bm = column(b_in[...], 0, hid), column(b_mid[...], 0, w_mid.shape[1])
    wi, wm = split(w_in[...].T), split(w_mid[...].T)
    width = w_out.shape[1]
    oh, ol = split(w_out[...])
    nt = ((1,), (1,))
    i = lax.broadcasted_iota(jnp.int32, (chans, width), 0)
    j = lax.broadcasted_iota(jnp.int32, (chans, width), 1)
    pick = jnp.where(j == i + first, 1.0, 0.0).astype(BF16)
    own = (mm(pick, oh, nt).astype(BF16), mm(pick, ol, nt).astype(BF16))
    dec = column(decay[...], first, chans)
    gain = jnp.sqrt(2.0 * dec / length)
    most = max(1, 2048 // inner)
    result = []
    for start, stop in parts:
        blocks = []
        for s0 in range(start, stop, most):
            some = range(s0, min(stop, s0 + most))
            cs, sn = [], []
            for s in some:
                a, b = sc[:, s : s + 1], ss[:, s : s + 1]
                cs.append(rc * a - rs * b)
                sn.append(rs * a + rc * b)
            feats = jnp.concatenate([jnp.concatenate(cs, 1), jnp.concatenate(sn, 1)], 0)
            h = jnp.maximum(dot3(wi, split(feats)) + bi, 0.0)
            h = jnp.maximum(dot3(wm, split(h)) + bm, 0.0)
            shape = dot3(own, split(h))
            n = (lax.broadcasted_iota(jnp.int32, shape.shape, 1) + s0 * inner).astype(F32) / length
            kern = shape * (jnp.exp(-dec * n) * gain)
            blocks += [kern[:, q * inner : (q + 1) * inner] for q in range(len(some))]
        result.append(blocks)
    return result


def body(
    n, m, groups,
    tok_hbm, gate_hbm, value_hbm, out_hbm, turn_hbm, mat_hbm,
    wave_hbm, w_in_hbm, b_in_hbm, w_mid_hbm, b_mid_hbm, w_out_hbm, decay_hbm,
    result,
    wave, w_in, b_in, w_mid, b_mid, w_out, decay,
    tok, gate_w, value_w, out_w, turn, mat,
    sent, got, got_x, own_out, own_in, cross_out, cross_in, spec_ref, prod_ref, w_high, w_low, part_out, part_in,
    up_sem, all_sem, far_sem, tok_recv, a_recv, x_recv, b_recv, y_recv, p_recv, load_sem, send_sems,
):
    tok_send, a_send, x_send, b_send, y_send, p_send = (send_sems.at[i] for i in range(6))
    me, mine = lax.axis_index("seq"), lax.axis_index("chan")
    rows, depth = tok_hbm.shape
    width = value_w.shape[1]
    half = n // 2
    side, idx = me // half, lax.rem(me, half)
    chans = width // half

    def flipped(at, i, count):
        if count & (count - 1):
            return lax.rem(at + i, count)
        bit, to = 1, 0
        while bit < count:
            here = lax.rem(at // bit, 2)
            to = to + (1 - here if i & bit else here) * bit
            bit *= 2
        return to

    loads = [
        pltpu.make_async_copy(src, dst, load_sem.at[i])
        for i, (src, dst) in enumerate(
            [
                (tok_hbm, tok.at[mine]), (value_hbm, value_w), (gate_hbm, gate_w), (mat_hbm, mat), (turn_hbm, turn), (out_hbm, out_w),
                (wave_hbm, wave), (w_in_hbm, w_in), (b_in_hbm, b_in), (w_mid_hbm, w_mid), (b_mid_hbm, b_mid), (w_out_hbm, w_out), (decay_hbm, decay),
            ]
        )
    ]
    for c in loads[:2]:
        c.start()

    barrier = pltpu.get_barrier_semaphore()
    lead, quarter = m - 1, half // 2
    lower, by_value = side == 0, mine == lead
    first_z, second_z = jnp.logical_and(lower, idx < quarter), jnp.logical_and(lower, idx >= quarter)
    by_result = jnp.logical_not(by_value)
    @pl.when(mine == lead)
    def _():
        pl.semaphore_signal(barrier, inc=1, device_id={"chan": 1 - lead}, device_id_type=MESH)

    for i in range(half - 1, 0, -1):
        to = side * half + flipped(idx, i, half)
        pl.semaphore_signal(barrier, inc=1, device_id={"seq": to, "chan": lead}, device_id_type=MESH)

    @pl.when(jnp.logical_not(lower))
    def _():
        for to in range(quarter, half):
            pl.semaphore_signal(barrier, inc=1, device_id={"seq": to, "chan": lead}, device_id_type=MESH)

    for c in loads[2:]:
        c.start()

    def remote(src, dst, send, recv, to):
        c = pltpu.make_async_remote_copy(
            src_ref=src, dst_ref=dst, send_sem=send, recv_sem=recv, device_id=to, device_id_type=MESH
        )
        c.start()
        return c

    def drain(block, sem):
        pltpu.make_async_copy(block, block, sem).wait()

    def peers(ref, g):
        return ref.at[pl.ds(0, half - 1), pl.ds(groups[g][0], groups[g][1]), :]

    def lines(ref, who, g):
        first, count = groups[g]
        return ref.at[pl.ds(pl.multiple_of(who * chans + first, 8), count), :]

    def weight(who, w_ref):
        return split(w_ref[pl.ds(pl.multiple_of(who * depth, 8), depth), :])

    def project(who, w_ref):
        return dot3(split(tok[who]), weight(who, w_ref))

    @pl.when(mine != lead)
    def _():
        pl.semaphore_wait(barrier, 1)
        pl.semaphore_signal(up_sem, inc=1, device_id={"chan": lead}, device_id_type=MESH)

    @pl.when(mine == lead)
    def _():
        pl.semaphore_wait(up_sem, 1)

    loads[0].wait()
    pieces = [pl.ds(first, depth // 2) for first in (0, depth // 2)]
    for i, piece in enumerate(pieces):
        part_of = tok.at[mine, :, piece]
        remote(part_of, part_of, tok_send, tok_recv.at[i], {"chan": 1 - mine})
    loads[1].wait()
    value_sum = project(mine, value_w)
    ahead = weight(1 - mine, value_w)
    for i, piece in enumerate(pieces):
        drain(tok.at[mine, :, piece], tok_recv.at[i])
        there = slice(i * (depth // 2), (i + 1) * (depth // 2))
        value_sum = value_sum + dot3(split(tok[1 - mine, :, there]), tuple(w[there] for w in ahead))
    sent[...] = silu(value_sum).T

    near = sorted(range(half), key=lambda i: (bin(i % max(1, half // 2)).count("1"), i))

    def tell(sem, **who):
        pl.semaphore_signal(sem, inc=1, device_id=who, device_id_type=MESH)

    def cross_values():
        for g, (first, count) in enumerate(groups):
            for i in near:
                to = flipped(idx, i, half)
                there = got_x.at[idx, pl.ds(first, count), :]
                remote(lines(sent, to, g), there, x_send, x_recv.at[g], {"seq": half + to})

    @pl.when(jnp.logical_and(by_value, jnp.logical_not(second_z)))
    def _():
        pl.semaphore_wait(barrier, m * (half - 1))
        tell(all_sem, chan=1 - lead)

        @pl.when(jnp.logical_and(lower, idx + quarter < half))
        def _():
            tell(all_sem, seq=idx + quarter, chan=1 - lead)

    @pl.when(jnp.logical_and(by_value, second_z))
    def _():
        pl.semaphore_wait(barrier, m * (n - 1))
        tell(far_sem, chan=1 - lead)

        @pl.when(idx >= quarter)
        def _():
            tell(far_sem, seq=idx - quarter)

        cross_values()

    @pl.when(by_result)
    def _():
        pl.semaphore_wait(all_sem, 1)

    for g, (first, count) in enumerate(groups):
        for i in range(half - 1, 0, -1):
            to = flipped(idx, i, half)
            there = got.at[idx, pl.ds(first, count), :]
            remote(lines(sent, to, g), there, a_send, a_recv.at[g], {"seq": side * half + to})
        got[idx, first : first + count, :] = lines(sent, idx, g)[...]

    @pl.when(jnp.logical_and(by_value, first_z))
    def _():
        pl.semaphore_wait(far_sem, 1)
        tell(far_sem, chan=1 - lead)
        cross_values()

    for c in loads[3:5] + loads[6:]:
        c.wait()
    low, high = position_blocks(
        n * rows, rows, [(0, half), (half, n)], idx * chans, chans, wave, w_in, b_in, w_mid, b_mid, w_out, decay
    )
    kern, k_cross = [], []
    for first, count in groups:
        own = forward([b[first : first + count] for b in low], turn, mat)
        far = forward([b[first : first + count] for b in high], turn, mat)
        kern.append(own)
        k_cross.append(jnp.concatenate([far[:, :rows] - own[:, rows:], far[:, rows:] + own[:, :rows]], axis=1))

    def part(ref, g):
        first, count = groups[g]
        return [ref[s, first : first + count, :] for s in range(half)]

    for g, (first, count) in enumerate(groups):
        drain(peers(got, g), a_recv.at[g])
        spec = forward(part(got, g), turn, mat)
        spec_ref[g] = spec
        prod_ref[g] = cmul(spec, kern[g])

        @pl.when(jnp.logical_and(side == 1, by_value))
        def _():
            drain(got_x.at[:, pl.ds(first, count), :], x_recv.at[g])
            prod_ref[g] = prod_ref[g] + cmul(forward(part(got_x, g), turn, mat), k_cross[g])

        for s, y in enumerate(backward(prod_ref[g], half, turn, mat)):
            own_out[s, first : first + count, :] = y
        for i in range(half - 1, 0, -1):
            to = flipped(idx, i, half)
            here, there = own_out.at[to, pl.ds(first, count), :], own_in.at[idx, pl.ds(first, count), :]
            remote(here, there, b_send, b_recv.at[g], {"seq": side * half + to})
        own_in[idx, first : first + count, :] = own_out[idx, first : first + count, :]

        @pl.when(jnp.logical_and(lower, by_result))
        def _():
            for s, y in enumerate(backward(cmul(spec_ref[g], k_cross[g]), half, turn, mat)):
                cross_out[s, first : first + count, :] = y
            if g == 0:
                pl.semaphore_wait(far_sem, 1)
            for i in reversed(near):
                to = flipped(idx, i, half)
                here, there = cross_out.at[to, pl.ds(first, count), :], cross_in.at[idx, pl.ds(first, count), :]
                remote(here, there, y_send, y_recv.at[g], {"seq": half + to})

    loads[2].wait()
    gate_sum = project(mine, gate_w)
    for i in range(1, m):
        gate_sum = gate_sum + project(lax.rem(mine + m - i, m), gate_w)
    gate_lines = silu(gate_sum).T.reshape(half, chans, rows)
    loads[5].wait()
    for g, (first, count) in enumerate(groups):
        some = out_w[...].reshape(half, chans, m * depth)[:, first : first + count, :]
        w_high[g], w_low[g] = split(some.reshape(half * count, m * depth))
    other = lax.rem(mine + 1, m)

    def partial(mixed, g, start, size):
        cols = pl.ds(pl.multiple_of(start, 128), size)
        return dot3(mixed, (w_high[g, :, cols], w_low[g, :, cols]))

    sums = [0.0, 0.0]
    for g, (first, count) in enumerate(groups):
        drain(peers(own_in, g), b_recv.at[g])

        @pl.when(jnp.logical_and(side == 1, by_result))
        def _():
            drain(cross_in.at[:, pl.ds(first, count), :], y_recv.at[g])
            own_in[:, first : first + count, :] = (
                own_in[:, first : first + count, :] + cross_in[:, first : first + count, :]
            )

        some = slice(first, first + count)
        mixed = split((gate_lines[:, some, :] * own_in[:, some, :]).reshape(half * count, rows).T)
        if g < len(groups) - 1:
            sums = [t + partial(mixed, g, who * depth, depth) for t, who in zip(sums, (mine, other))]

    part_out[...] = sums[1] + partial(mixed, len(groups) - 1, other * depth, depth)
    remote(part_out, part_in, p_send, p_recv, {"chan": other})
    total = sums[0] + partial(mixed, len(groups) - 1, mine * depth, depth)
    drain(part_in, p_recv)
    result[...] = total + part_in[...]
    for g in range(len(groups)):
        drain(peers(got, g), a_send)
        drain(peers(own_in, g), b_send)

    @pl.when(jnp.logical_and(lower, by_value))
    def _():
        drain(got_x, x_send)

    @pl.when(jnp.logical_and(lower, by_result))
    def _():
        drain(cross_out, y_send)

    drain(tok.at[mine], tok_send)
    drain(part_out, p_send)


def scoped_body(*args):
    pl.run_scoped(
        functools.partial(body, *args), pltpu.SemaphoreType.DMA((13,)), pltpu.SemaphoreType.DMA((6,))
    )


def on_device(
    tokens, gate_weight, value_weight, output_weight, wave_numbers,
    position_in, bias_in, position_mid, bias_mid, position_out, decay_rate,
):
    n, m = lax.axis_size("seq"), lax.axis_size("chan")
    rows, depth = tokens.shape
    width = gate_weight.shape[1]
    half = n // 2
    chans = width // half
    count = chans // 2 if chans % 16 == 0 else chans
    groups = [(first, count) for first in range(0, chans, count)]
    assert m == 2 and n % 2 == 0
    turns, mats = tables(half, rows)
    hbm = pl.BlockSpec(memory_space=pl.ANY)
    vmem = pl.BlockSpec(memory_space=pltpu.VMEM)
    dma = pltpu.SemaphoreType.DMA
    return pl.pallas_call(
        functools.partial(scoped_body, n, m, groups),
        out_shape=pltpu.VMEM((rows, depth), F32),
        in_specs=[hbm] * 13,
        out_specs=vmem,
        scratch_shapes=[
            pltpu.VMEM((1, wave_numbers.shape[0]), jnp.int32),
            pltpu.VMEM(position_in.shape, F32),
            pltpu.VMEM((1, bias_in.shape[0]), F32),
            pltpu.VMEM(position_mid.shape, F32),
            pltpu.VMEM((1, bias_mid.shape[0]), F32),
            pltpu.VMEM(position_out.shape, F32),
            pltpu.VMEM((1, width), F32),
            pltpu.VMEM((m, rows, depth), F32),
            pltpu.VMEM(gate_weight.shape, F32),
            pltpu.VMEM(value_weight.shape, F32),
            pltpu.VMEM(output_weight.shape, F32),
            pltpu.VMEM(turns.shape, F32),
            pltpu.VMEM(mats.shape, BF16),
            pltpu.VMEM((width, rows), F32),
            pltpu.VMEM((half, chans, rows), F32),
            pltpu.VMEM((half, chans, rows), F32),
            pltpu.VMEM((half, chans, rows), F32),
            pltpu.VMEM((half, chans, rows), F32),
            pltpu.VMEM((half, chans, rows), F32),
            pltpu.VMEM((half, chans, rows), F32),
            pltpu.VMEM((len(groups), half * count, 2 * rows), F32),
            pltpu.VMEM((len(groups), half * count, 2 * rows), F32),
            pltpu.VMEM((len(groups), half * count, m * depth), BF16),
            pltpu.VMEM((len(groups), half * count, m * depth), BF16),
            pltpu.VMEM((rows, depth), F32),
            pltpu.VMEM((rows, depth), F32),
            pltpu.SemaphoreType.REGULAR,
            pltpu.SemaphoreType.REGULAR,
            pltpu.SemaphoreType.REGULAR,
            dma((2,)),
            dma((len(groups),)), dma((len(groups),)), dma((len(groups),)), dma((len(groups),)),
            dma,
        ],
        compiler_params=pltpu.CompilerParams(collective_id=0, has_side_effects=True),
    )(
        tokens, gate_weight, value_weight, output_weight, jnp.asarray(turns), jnp.asarray(mats),
        wave_numbers[None, :], position_in, bias_in[None, :], position_mid, bias_mid[None, :],
        position_out, decay_rate[None, :],
    )


def solution(mesh):
    placed = (
        P("seq", "chan"), P(None, "chan"), P(None, "chan"), P("chan", None),
        P(), P(), P(), P(), P(), P(None, "chan"), P("chan"),
    )
    return jax.shard_map(
        on_device, mesh=mesh, in_specs=placed, out_specs=P("seq", "chan"), check_vma=False
    )
```

```python
import functools
import math

import jax
import jax.numpy as jnp
import numpy as np
from jax import lax
from jax.experimental import pallas as pl
from jax.experimental.pallas import tpu as pltpu
from jax.sharding import PartitionSpec as P

PERIOD = 4096
F32 = jnp.float32
BF16 = jnp.bfloat16
MESH = pl.DeviceIdType.MESH


def split(a):
    hi = a.astype(BF16)
    return hi, (a - hi.astype(F32)).astype(BF16)


def mm(a, b, dims=((1,), (0,))):
    return lax.dot_general(a, b, (dims, ((), ())), preferred_element_type=F32)


def dot3(a, b, dims=((1,), (0,))):
    (ah, al), (bh, bl) = a, b
    return mm(ah, bh, dims) + (mm(ah, bl, dims) + mm(al, bh, dims))


def silu(v):
    return v / (1.0 + jnp.exp(-v))


def cmul_const(z, angle):
    c, s = math.cos(angle), math.sin(angle)
    re, im = z
    if abs(s) < 1e-12:
        return (re, im) if c > 0 else (-re, -im)
    if abs(c) < 1e-12:
        return (-im, re) if s > 0 else (im, -re)
    return (re * c - im * s, re * s + im * c)


def fft(xs, sign):
    n = len(xs)
    if n == 1:
        return xs
    even, odd = fft(xs[0::2], sign), fft(xs[1::2], sign)
    low, high = [], []
    for k in range(n // 2):
        er, ei = even[k]
        tr, ti = cmul_const(odd[k], sign * 2.0 * math.pi * k / n)
        low.append((er + tr, ei + ti))
        high.append((er - tr, ei - ti))
    return low + high


def tables(outer, inner):
    length = outer * inner
    r = np.arange(inner)
    turn = 2.0 * np.pi * np.outer(np.arange(outer) + 0.25, r) / length
    turns = np.concatenate([np.cos(turn), np.sin(turn)], 0).astype(np.float32)
    ang = 2.0 * np.pi * (np.outer(r, r) % inner) / inner
    c, s = np.cos(ang), np.sin(ang)
    fwd = np.block([[c, -s], [s, c]]).astype(np.float32)
    inv = (np.block([[c, s], [-s, c]]) / length).astype(np.float32)

    def halves(a):
        hi = a.astype(jnp.bfloat16)
        return [hi, (a - hi.astype(np.float32)).astype(jnp.bfloat16)]

    return turns, np.stack(halves(fwd) + halves(inv))


def column(row, first, count):
    n = row.shape[1]
    i = lax.broadcasted_iota(jnp.int32, (count, n), 0)
    j = lax.broadcasted_iota(jnp.int32, (count, n), 1)
    picked = jnp.where(j == i + first, jnp.broadcast_to(row, (count, n)), jnp.zeros_like(row))
    return jnp.sum(picked, axis=1, keepdims=True)


def forward(blocks, turn_ref, mat_ref):
    outer = len(blocks)
    step = -2.0 * math.pi / (4 * outer)
    twisted = [(b * math.cos(step * s), b * math.sin(step * s)) if s else (b, None) for s, b in enumerate(blocks)]
    twisted[0] = (blocks[0], jnp.zeros_like(blocks[0]))
    rows = []
    for k, (re, im) in enumerate(fft(twisted, -1.0)):
        c, s = turn_ref[k : k + 1, :], turn_ref[outer + k : outer + k + 1, :]
        rows.append(jnp.concatenate([re * c + im * s, im * c - re * s], axis=1))
    grid = jnp.concatenate(rows, axis=0)
    return dot3(split(grid), (mat_ref[0], mat_ref[1]))


def backward(spectrum, outer, turn_ref, mat_ref):
    back = dot3(split(spectrum), (mat_ref[2], mat_ref[3]))
    chans, inner = spectrum.shape[0] // outer, spectrum.shape[1] // 2
    zs = []
    for k in range(outer):
        re = back[k * chans : (k + 1) * chans, :inner]
        im = back[k * chans : (k + 1) * chans, inner:]
        c, s = turn_ref[k : k + 1, :], turn_ref[outer + k : outer + k + 1, :]
        zs.append((re * c - im * s, re * s + im * c))
    ys = fft(zs, 1.0)
    step = 2.0 * math.pi / (4 * outer)
    return [re * math.cos(step * s) - im * math.sin(step * s) for s, (re, im) in enumerate(ys)]


def cmul(a, b):
    half = a.shape[1] // 2
    ar, ai, br, bi = a[:, :half], a[:, half:], b[:, :half], b[:, half:]
    return jnp.concatenate([ar * br - ai * bi, ar * bi + ai * br], axis=1)


def position_blocks(length, inner, parts, first, chans, wave, w_in, b_in, w_mid, b_mid, w_out, decay):
    waves = wave.shape[1]
    hid = w_in.shape[1]
    wcol = column(wave[...], 0, waves)
    unit = 2.0 * math.pi / PERIOD

    def trig(spots):
        ang = (lax.rem(spots * wcol, PERIOD)).astype(F32) * unit
        return jnp.cos(ang), jnp.sin(ang)

    rc, rs = trig(lax.broadcasted_iota(jnp.int32, (waves, inner), 1))
    sc, ss = trig(lax.broadcasted_iota(jnp.int32, (waves, max(length // inner, 128)), 1) * inner)
    bi, bm = column(b_in[...], 0, hid), column(b_mid[...], 0, w_mid.shape[1])
    wi, wm = split(w_in[...].T), split(w_mid[...].T)
    width = w_out.shape[1]
    oh, ol = split(w_out[...])
    nt = ((1,), (1,))
    i = lax.broadcasted_iota(jnp.int32, (chans, width), 0)
    j = lax.broadcasted_iota(jnp.int32, (chans, width), 1)
    pick = jnp.where(j == i + first, 1.0, 0.0).astype(BF16)
    own = (mm(pick, oh, nt).astype(BF16), mm(pick, ol, nt).astype(BF16))
    dec = column(decay[...], first, chans)
    gain = jnp.sqrt(2.0 * dec / length)
    most = max(1, 2048 // inner)
    result = []
    for start, stop in parts:
        blocks = []
        for s0 in range(start, stop, most):
            some = range(s0, min(stop, s0 + most))
            cs, sn = [], []
            for s in some:
                a, b = sc[:, s : s + 1], ss[:, s : s + 1]
                cs.append(rc * a - rs * b)
                sn.append(rs * a + rc * b)
            feats = jnp.concatenate([jnp.concatenate(cs, 1), jnp.concatenate(sn, 1)], 0)
            h = jnp.maximum(dot3(wi, split(feats)) + bi, 0.0)
            h = jnp.maximum(dot3(wm, split(h)) + bm, 0.0)
            shape = dot3(own, split(h))
            n = (lax.broadcasted_iota(jnp.int32, shape.shape, 1) + s0 * inner).astype(F32) / length
            kern = shape * (jnp.exp(-dec * n) * gain)
            blocks += [kern[:, q * inner : (q + 1) * inner] for q in range(len(some))]
        result.append(blocks)
    return result


def body(
    n, m, groups,
    tok_hbm, gate_hbm, value_hbm, out_hbm, turn_hbm, mat_hbm,
    wave_hbm, w_in_hbm, b_in_hbm, w_mid_hbm, b_mid_hbm, w_out_hbm, decay_hbm,
    result,
    wave, w_in, b_in, w_mid, b_mid, w_out, decay,
    tok, gate_w, value_w, out_w, turn, mat,
    sent, got, got_x, own_out, own_in, cross_out, cross_in, spec_ref, prod_ref, w_high, w_low, part_out, part_in,
    up_sem, all_sem, near_sem, far_sem, tok_recv, a_recv, x_recv, b_recv, y_recv, p_recv, load_sem, send_sems,
):
    tok_send, a_send, x_send, b_send, y_send, p_send = (send_sems.at[i] for i in range(6))
    me, mine = lax.axis_index("seq"), lax.axis_index("chan")
    rows, depth = tok_hbm.shape
    width = value_w.shape[1]
    half = n // 2
    side, idx = me // half, lax.rem(me, half)
    chans = width // half

    def flipped(at, i, count):
        if count & (count - 1):
            return lax.rem(at + i, count)
        bit, to = 1, 0
        while bit < count:
            here = lax.rem(at // bit, 2)
            to = to + (1 - here if i & bit else here) * bit
            bit *= 2
        return to

    loads = [
        pltpu.make_async_copy(src, dst, load_sem.at[i])
        for i, (src, dst) in enumerate(
            [
                (tok_hbm, tok.at[mine]), (value_hbm, value_w), (gate_hbm, gate_w), (mat_hbm, mat), (turn_hbm, turn), (out_hbm, out_w),
                (wave_hbm, wave), (w_in_hbm, w_in), (b_in_hbm, b_in), (w_mid_hbm, w_mid), (b_mid_hbm, b_mid), (w_out_hbm, w_out), (decay_hbm, decay),
            ]
        )
    ]
    for c in loads[:2]:
        c.start()

    barrier = pltpu.get_barrier_semaphore()
    lead, quarter = m - 1, half // 2
    lower, by_value = side == 0, mine == lead
    first_z, second_z = jnp.logical_and(lower, idx < quarter), jnp.logical_and(lower, idx >= quarter)
    third_z = jnp.logical_and(side == 1, idx < quarter)
    by_result = jnp.logical_not(by_value)
    @pl.when(mine == lead)
    def _():
        pl.semaphore_signal(barrier, inc=1, device_id={"chan": 1 - lead}, device_id_type=MESH)

    for i in range(half - 1, 0, -1):
        to = side * half + flipped(idx, i, half)
        pl.semaphore_signal(barrier, inc=1, device_id={"seq": to, "chan": lead}, device_id_type=MESH)

    @pl.when(third_z)
    def _():
        for to in range(quarter, half):
            pl.semaphore_signal(barrier, inc=1, device_id={"seq": to, "chan": lead}, device_id_type=MESH)

    @pl.when(second_z)
    def _():
        to = me + quarter
        pl.semaphore_signal(barrier, inc=1, device_id={"seq": to, "chan": lead}, device_id_type=MESH)

    for c in loads[2:]:
        c.start()

    def remote(src, dst, send, recv, to):
        c = pltpu.make_async_remote_copy(
            src_ref=src, dst_ref=dst, send_sem=send, recv_sem=recv, device_id=to, device_id_type=MESH
        )
        c.start()
        return c

    def drain(block, sem):
        pltpu.make_async_copy(block, block, sem).wait()

    def peers(ref, g):
        return ref.at[pl.ds(0, half - 1), pl.ds(groups[g][0], groups[g][1]), :]

    def lines(ref, who, g):
        first, count = groups[g]
        return ref.at[pl.ds(pl.multiple_of(who * chans + first, 8), count), :]

    def weight(who, w_ref):
        return split(w_ref[pl.ds(pl.multiple_of(who * depth, 8), depth), :])

    def project(who, w_ref):
        return dot3(split(tok[who]), weight(who, w_ref))

    @pl.when(mine != lead)
    def _():
        pl.semaphore_wait(barrier, 1)
        pl.semaphore_signal(up_sem, inc=1, device_id={"chan": lead}, device_id_type=MESH)

    @pl.when(mine == lead)
    def _():
        pl.semaphore_wait(up_sem, 1)

    loads[0].wait()
    pieces = [pl.ds(first, depth // 2) for first in (0, depth // 2)]
    for i, piece in enumerate(pieces):
        part_of = tok.at[mine, :, piece]
        remote(part_of, part_of, tok_send, tok_recv.at[i], {"chan": 1 - mine})
    loads[1].wait()
    value_sum = project(mine, value_w)
    ahead = weight(1 - mine, value_w)
    for i, piece in enumerate(pieces):
        drain(tok.at[mine, :, piece], tok_recv.at[i])
        there = slice(i * (depth // 2), (i + 1) * (depth // 2))
        value_sum = value_sum + dot3(split(tok[1 - mine, :, there]), tuple(w[there] for w in ahead))
    sent[...] = silu(value_sum).T

    near = sorted(range(half), key=lambda i: (bin(i % max(1, half // 2)).count("1"), i))

    def tell(sem, **who):
        pl.semaphore_signal(sem, inc=1, device_id=who, device_id_type=MESH)

    def cross_values(some):
        for g, (first, count) in enumerate(groups):
            for i in sorted(range(quarter), key=lambda i: bin(i).count("1")):
                to = some + flipped(lax.rem(idx, quarter), i, quarter)
                there = got_x.at[idx, pl.ds(first, count), :]
                remote(lines(sent, to, g), there, x_send, x_recv.at[g], {"seq": half + to})

    @pl.when(jnp.logical_and(by_value, jnp.logical_not(jnp.logical_or(second_z, third_z))))
    def _():
        pl.semaphore_wait(barrier, m * (half - 1))
        tell(all_sem, chan=1 - lead)

        @pl.when(lower)
        def _():
            tell(all_sem, seq=me + quarter, chan=1 - lead)

    @pl.when(jnp.logical_and(by_value, third_z))
    def _():
        pl.semaphore_wait(barrier, m * half)
        tell(all_sem, chan=1 - lead)
        tell(far_sem, seq=me - quarter)

    @pl.when(jnp.logical_and(by_value, second_z))
    def _():
        pl.semaphore_wait(barrier, m * (half - 1 + quarter))
        tell(near_sem, seq=me - quarter)
        cross_values(0)
        pl.semaphore_wait(far_sem, 1)
        tell(far_sem, chan=1 - lead)
        tell(far_sem, seq=me - quarter)
        cross_values(quarter)

    @pl.when(by_result)
    def _():
        pl.semaphore_wait(all_sem, 1)

    for g, (first, count) in enumerate(groups):
        for i in range(half - 1, 0, -1):
            to = flipped(idx, i, half)
            there = got.at[idx, pl.ds(first, count), :]
            remote(lines(sent, to, g), there, a_send, a_recv.at[g], {"seq": side * half + to})
        got[idx, first : first + count, :] = lines(sent, idx, g)[...]

    @pl.when(jnp.logical_and(by_value, first_z))
    def _():
        pl.semaphore_wait(near_sem, 1)
        cross_values(0)
        pl.semaphore_wait(far_sem, 1)
        tell(far_sem, chan=1 - lead)
        cross_values(quarter)

    for c in loads[3:5] + loads[6:]:
        c.wait()
    low, high = position_blocks(
        n * rows, rows, [(0, half), (half, n)], idx * chans, chans, wave, w_in, b_in, w_mid, b_mid, w_out, decay
    )
    kern, k_cross = [], []
    for first, count in groups:
        own = forward([b[first : first + count] for b in low], turn, mat)
        far = forward([b[first : first + count] for b in high], turn, mat)
        kern.append(own)
        k_cross.append(jnp.concatenate([far[:, :rows] - own[:, rows:], far[:, rows:] + own[:, :rows]], axis=1))

    def part(ref, g):
        first, count = groups[g]
        return [ref[s, first : first + count, :] for s in range(half)]

    for g, (first, count) in enumerate(groups):
        drain(peers(got, g), a_recv.at[g])
        spec = forward(part(got, g), turn, mat)
        spec_ref[g] = spec
        prod_ref[g] = cmul(spec, kern[g])

        @pl.when(jnp.logical_and(side == 1, by_value))
        def _():
            drain(got_x.at[:, pl.ds(first, count), :], x_recv.at[g])
            prod_ref[g] = prod_ref[g] + cmul(forward(part(got_x, g), turn, mat), k_cross[g])

        for s, y in enumerate(backward(prod_ref[g], half, turn, mat)):
            own_out[s, first : first + count, :] = y
        for i in range(half - 1, 0, -1):
            to = flipped(idx, i, half)
            here, there = own_out.at[to, pl.ds(first, count), :], own_in.at[idx, pl.ds(first, count), :]
            remote(here, there, b_send, b_recv.at[g], {"seq": side * half + to})
        own_in[idx, first : first + count, :] = own_out[idx, first : first + count, :]

        @pl.when(jnp.logical_and(lower, by_result))
        def _():
            for s, y in enumerate(backward(cmul(spec_ref[g], k_cross[g]), half, turn, mat)):
                cross_out[s, first : first + count, :] = y
            if g == 0:
                pl.semaphore_wait(far_sem, 1)
            for i in reversed(near):
                to = flipped(idx, i, half)
                here, there = cross_out.at[to, pl.ds(first, count), :], cross_in.at[idx, pl.ds(first, count), :]
                remote(here, there, y_send, y_recv.at[g], {"seq": half + to})

    loads[2].wait()
    gate_sum = project(mine, gate_w)
    for i in range(1, m):
        gate_sum = gate_sum + project(lax.rem(mine + m - i, m), gate_w)
    gate_lines = silu(gate_sum).T.reshape(half, chans, rows)
    loads[5].wait()
    for g, (first, count) in enumerate(groups):
        some = out_w[...].reshape(half, chans, m * depth)[:, first : first + count, :]
        w_high[g], w_low[g] = split(some.reshape(half * count, m * depth))
    other = lax.rem(mine + 1, m)

    def partial(mixed, g, start, size):
        cols = pl.ds(pl.multiple_of(start, 128), size)
        return dot3(mixed, (w_high[g, :, cols], w_low[g, :, cols]))

    sums = [0.0, 0.0]
    for g, (first, count) in enumerate(groups):
        drain(peers(own_in, g), b_recv.at[g])

        @pl.when(jnp.logical_and(side == 1, by_result))
        def _():
            drain(cross_in.at[:, pl.ds(first, count), :], y_recv.at[g])
            own_in[:, first : first + count, :] = (
                own_in[:, first : first + count, :] + cross_in[:, first : first + count, :]
            )

        some = slice(first, first + count)
        mixed = split((gate_lines[:, some, :] * own_in[:, some, :]).reshape(half * count, rows).T)
        if g < len(groups) - 1:
            sums = [t + partial(mixed, g, who * depth, depth) for t, who in zip(sums, (mine, other))]

    part_out[...] = sums[1] + partial(mixed, len(groups) - 1, other * depth, depth)
    remote(part_out, part_in, p_send, p_recv, {"chan": other})
    total = sums[0] + partial(mixed, len(groups) - 1, mine * depth, depth)
    drain(part_in, p_recv)
    result[...] = total + part_in[...]
    for g in range(len(groups)):
        drain(peers(got, g), a_send)
        drain(peers(own_in, g), b_send)

    @pl.when(jnp.logical_and(lower, by_value))
    def _():
        drain(got_x, x_send)

    @pl.when(jnp.logical_and(lower, by_result))
    def _():
        drain(cross_out, y_send)

    drain(tok.at[mine], tok_send)
    drain(part_out, p_send)


def scoped_body(*args):
    pl.run_scoped(
        functools.partial(body, *args), pltpu.SemaphoreType.DMA((13,)), pltpu.SemaphoreType.DMA((6,))
    )


def on_device(
    tokens, gate_weight, value_weight, output_weight, wave_numbers,
    position_in, bias_in, position_mid, bias_mid, position_out, decay_rate,
):
    n, m = lax.axis_size("seq"), lax.axis_size("chan")
    rows, depth = tokens.shape
    width = gate_weight.shape[1]
    half = n // 2
    chans = width // half
    count = chans // 2 if chans % 16 == 0 else chans
    groups = [(first, count) for first in range(0, chans, count)]
    assert m == 2 and n % 4 == 0
    turns, mats = tables(half, rows)
    hbm = pl.BlockSpec(memory_space=pl.ANY)
    vmem = pl.BlockSpec(memory_space=pltpu.VMEM)
    dma = pltpu.SemaphoreType.DMA
    return pl.pallas_call(
        functools.partial(scoped_body, n, m, groups),
        out_shape=pltpu.VMEM((rows, depth), F32),
        in_specs=[hbm] * 13,
        out_specs=vmem,
        scratch_shapes=[
            pltpu.VMEM((1, wave_numbers.shape[0]), jnp.int32),
            pltpu.VMEM(position_in.shape, F32),
            pltpu.VMEM((1, bias_in.shape[0]), F32),
            pltpu.VMEM(position_mid.shape, F32),
            pltpu.VMEM((1, bias_mid.shape[0]), F32),
            pltpu.VMEM(position_out.shape, F32),
            pltpu.VMEM((1, width), F32),
            pltpu.VMEM((m, rows, depth), F32),
            pltpu.VMEM(gate_weight.shape, F32),
            pltpu.VMEM(value_weight.shape, F32),
            pltpu.VMEM(output_weight.shape, F32),
            pltpu.VMEM(turns.shape, F32),
            pltpu.VMEM(mats.shape, BF16),
            pltpu.VMEM((width, rows), F32),
            pltpu.VMEM((half, chans, rows), F32),
            pltpu.VMEM((half, chans, rows), F32),
            pltpu.VMEM((half, chans, rows), F32),
            pltpu.VMEM((half, chans, rows), F32),
            pltpu.VMEM((half, chans, rows), F32),
            pltpu.VMEM((half, chans, rows), F32),
            pltpu.VMEM((len(groups), half * count, 2 * rows), F32),
            pltpu.VMEM((len(groups), half * count, 2 * rows), F32),
            pltpu.VMEM((len(groups), half * count, m * depth), BF16),
            pltpu.VMEM((len(groups), half * count, m * depth), BF16),
            pltpu.VMEM((rows, depth), F32),
            pltpu.VMEM((rows, depth), F32),
            pltpu.SemaphoreType.REGULAR,
            pltpu.SemaphoreType.REGULAR,
            pltpu.SemaphoreType.REGULAR,
            pltpu.SemaphoreType.REGULAR,
            dma((2,)),
            dma((len(groups),)), dma((len(groups),)), dma((len(groups),)), dma((len(groups),)),
            dma,
        ],
        compiler_params=pltpu.CompilerParams(collective_id=0, has_side_effects=True),
    )(
        tokens, gate_weight, value_weight, output_weight, jnp.asarray(turns), jnp.asarray(mats),
        wave_numbers[None, :], position_in, bias_in[None, :], position_mid, bias_mid[None, :],
        position_out, decay_rate[None, :],
    )


def solution(mesh):
    placed = (
        P("seq", "chan"), P(None, "chan"), P(None, "chan"), P("chan", None),
        P(), P(), P(), P(), P(), P(None, "chan"), P("chan"),
    )
    return jax.shard_map(
        on_device, mesh=mesh, in_specs=placed, out_specs=P("seq", "chan"), check_vma=False
    )
```

```python
import functools
import math

import jax
import jax.numpy as jnp
import numpy as np
from jax import lax
from jax.experimental import pallas as pl
from jax.experimental.pallas import tpu as pltpu
from jax.sharding import PartitionSpec as P

PERIOD = 4096
F32 = jnp.float32
BF16 = jnp.bfloat16
MESH = pl.DeviceIdType.MESH


def split(a):
    hi = a.astype(BF16)
    return hi, (a - hi.astype(F32)).astype(BF16)


def mm(a, b, dims=((1,), (0,))):
    return lax.dot_general(a, b, (dims, ((), ())), preferred_element_type=F32)


def dot3(a, b, dims=((1,), (0,))):
    (ah, al), (bh, bl) = a, b
    return mm(ah, bh, dims) + (mm(ah, bl, dims) + mm(al, bh, dims))


def silu(v):
    return v / (1.0 + jnp.exp(-v))


def cmul_const(z, angle):
    c, s = math.cos(angle), math.sin(angle)
    re, im = z
    if abs(s) < 1e-12:
        return (re, im) if c > 0 else (-re, -im)
    if abs(c) < 1e-12:
        return (-im, re) if s > 0 else (im, -re)
    return (re * c - im * s, re * s + im * c)


def fft(xs, sign):
    n = len(xs)
    if n == 1:
        return xs
    even, odd = fft(xs[0::2], sign), fft(xs[1::2], sign)
    low, high = [], []
    for k in range(n // 2):
        er, ei = even[k]
        tr, ti = cmul_const(odd[k], sign * 2.0 * math.pi * k / n)
        low.append((er + tr, ei + ti))
        high.append((er - tr, ei - ti))
    return low + high


def tables(outer, inner):
    length = outer * inner
    r = np.arange(inner)
    turn = 2.0 * np.pi * np.outer(np.arange(outer) + 0.25, r) / length
    turns = np.concatenate([np.cos(turn), np.sin(turn)], 0).astype(np.float32)
    ang = 2.0 * np.pi * (np.outer(r, r) % inner) / inner
    c, s = np.cos(ang), np.sin(ang)
    fwd = np.block([[c, -s], [s, c]]).astype(np.float32)
    inv = (np.block([[c, s], [-s, c]]) / length).astype(np.float32)

    def halves(a):
        hi = a.astype(jnp.bfloat16)
        return [hi, (a - hi.astype(np.float32)).astype(jnp.bfloat16)]

    return turns, np.stack(halves(fwd) + halves(inv))


def column(row, first, count):
    n = row.shape[1]
    i = lax.broadcasted_iota(jnp.int32, (count, n), 0)
    j = lax.broadcasted_iota(jnp.int32, (count, n), 1)
    picked = jnp.where(j == i + first, jnp.broadcast_to(row, (count, n)), jnp.zeros_like(row))
    return jnp.sum(picked, axis=1, keepdims=True)


def forward(blocks, turn_ref, mat_ref):
    outer = len(blocks)
    step = -2.0 * math.pi / (4 * outer)
    twisted = [(b * math.cos(step * s), b * math.sin(step * s)) if s else (b, None) for s, b in enumerate(blocks)]
    twisted[0] = (blocks[0], jnp.zeros_like(blocks[0]))
    rows = []
    for k, (re, im) in enumerate(fft(twisted, -1.0)):
        c, s = turn_ref[k : k + 1, :], turn_ref[outer + k : outer + k + 1, :]
        rows.append(jnp.concatenate([re * c + im * s, im * c - re * s], axis=1))
    grid = jnp.concatenate(rows, axis=0)
    return dot3(split(grid), (mat_ref[0], mat_ref[1]))


def backward(spectrum, outer, turn_ref, mat_ref):
    back = dot3(split(spectrum), (mat_ref[2], mat_ref[3]))
    chans, inner = spectrum.shape[0] // outer, spectrum.shape[1] // 2
    zs = []
    for k in range(outer):
        re = back[k * chans : (k + 1) * chans, :inner]
        im = back[k * chans : (k + 1) * chans, inner:]
        c, s = turn_ref[k : k + 1, :], turn_ref[outer + k : outer + k + 1, :]
        zs.append((re * c - im * s, re * s + im * c))
    ys = fft(zs, 1.0)
    step = 2.0 * math.pi / (4 * outer)
    return [re * math.cos(step * s) - im * math.sin(step * s) for s, (re, im) in enumerate(ys)]


def cmul(a, b):
    half = a.shape[1] // 2
    ar, ai, br, bi = a[:, :half], a[:, half:], b[:, :half], b[:, half:]
    return jnp.concatenate([ar * br - ai * bi, ar * bi + ai * br], axis=1)


def position_blocks(length, inner, parts, first, chans, wave, w_in, b_in, w_mid, b_mid, w_out, decay):
    waves = wave.shape[1]
    hid = w_in.shape[1]
    wcol = column(wave[...], 0, waves)
    unit = 2.0 * math.pi / PERIOD

    def trig(spots):
        ang = (lax.rem(spots * wcol, PERIOD)).astype(F32) * unit
        return jnp.cos(ang), jnp.sin(ang)

    rc, rs = trig(lax.broadcasted_iota(jnp.int32, (waves, inner), 1))
    sc, ss = trig(lax.broadcasted_iota(jnp.int32, (waves, max(length // inner, 128)), 1) * inner)
    bi, bm = column(b_in[...], 0, hid), column(b_mid[...], 0, w_mid.shape[1])
    wi, wm = split(w_in[...].T), split(w_mid[...].T)
    width = w_out.shape[1]
    oh, ol = split(w_out[...])
    nt = ((1,), (1,))
    i = lax.broadcasted_iota(jnp.int32, (chans, width), 0)
    j = lax.broadcasted_iota(jnp.int32, (chans, width), 1)
    pick = jnp.where(j == i + first, 1.0, 0.0).astype(BF16)
    own = (mm(pick, oh, nt).astype(BF16), mm(pick, ol, nt).astype(BF16))
    dec = column(decay[...], first, chans)
    gain = jnp.sqrt(2.0 * dec / length)
    most = max(1, 2048 // inner)
    result = []
    for start, stop in parts:
        blocks = []
        for s0 in range(start, stop, most):
            some = range(s0, min(stop, s0 + most))
            cs, sn = [], []
            for s in some:
                a, b = sc[:, s : s + 1], ss[:, s : s + 1]
                cs.append(rc * a - rs * b)
                sn.append(rs * a + rc * b)
            feats = jnp.concatenate([jnp.concatenate(cs, 1), jnp.concatenate(sn, 1)], 0)
            h = jnp.maximum(dot3(wi, split(feats)) + bi, 0.0)
            h = jnp.maximum(dot3(wm, split(h)) + bm, 0.0)
            shape = dot3(own, split(h))
            n = (lax.broadcasted_iota(jnp.int32, shape.shape, 1) + s0 * inner).astype(F32) / length
            kern = shape * (jnp.exp(-dec * n) * gain)
            blocks += [kern[:, q * inner : (q + 1) * inner] for q in range(len(some))]
        result.append(blocks)
    return result


def body(
    n, m, groups,
    tok_hbm, gate_hbm, value_hbm, out_hbm, turn_hbm, mat_hbm,
    wave_hbm, w_in_hbm, b_in_hbm, w_mid_hbm, b_mid_hbm, w_out_hbm, decay_hbm,
    result,
    wave, w_in, b_in, w_mid, b_mid, w_out, decay,
    tok, gate_w, value_w, out_w, turn, mat,
    sent, got, got_x, own_out, own_in, cross_out, cross_in, spec_ref, prod_ref, w_high, w_low, part_out, part_in,
    up_sem, all_sem, near_sem, far_sem, tok_recv, a_recv, x_recv, b_recv, y_recv, p_recv, load_sem, send_sems,
):
    tok_send, a_send, x_send, b_send, y_send, p_send = (send_sems.at[i] for i in range(6))
    me, mine = lax.axis_index("seq"), lax.axis_index("chan")
    rows, depth = tok_hbm.shape
    width = value_w.shape[1]
    half = n // 2
    side, idx = me // half, lax.rem(me, half)
    chans = width // half

    def flipped(at, i, count):
        if count & (count - 1):
            return lax.rem(at + i, count)
        bit, to = 1, 0
        while bit < count:
            here = lax.rem(at // bit, 2)
            to = to + (1 - here if i & bit else here) * bit
            bit *= 2
        return to

    pieces = [pl.ds(first, depth // 2) for first in (0, depth // 2)]
    loads = [
        pltpu.make_async_copy(src, dst, load_sem.at[i])
        for i, (src, dst) in enumerate(
            [
                (tok_hbm.at[:, pieces[0]], tok.at[mine, :, pieces[0]]), (value_hbm, value_w), (gate_hbm, gate_w), (mat_hbm, mat), (turn_hbm, turn), (out_hbm, out_w),
                (wave_hbm, wave), (w_in_hbm, w_in), (b_in_hbm, b_in), (w_mid_hbm, w_mid), (b_mid_hbm, b_mid), (w_out_hbm, w_out), (decay_hbm, decay),
                (tok_hbm.at[:, pieces[1]], tok.at[mine, :, pieces[1]]),
            ]
        )
    ]
    for c in (loads[0], loads[13], loads[1]):
        c.start()

    barrier = pltpu.get_barrier_semaphore()
    lead, quarter = m - 1, half // 2
    lower, by_value = side == 0, mine == lead
    first_z, second_z = jnp.logical_and(lower, idx < quarter), jnp.logical_and(lower, idx >= quarter)
    third_z = jnp.logical_and(side == 1, idx < quarter)
    by_result = jnp.logical_not(by_value)
    @pl.when(mine == lead)
    def _():
        pl.semaphore_signal(barrier, inc=1, device_id={"chan": 1 - lead}, device_id_type=MESH)

    for i in range(half - 1, 0, -1):
        to = side * half + flipped(idx, i, half)
        pl.semaphore_signal(barrier, inc=1, device_id={"seq": to, "chan": lead}, device_id_type=MESH)

    @pl.when(third_z)
    def _():
        for to in range(quarter, half):
            pl.semaphore_signal(barrier, inc=1, device_id={"seq": to, "chan": lead}, device_id_type=MESH)

    @pl.when(second_z)
    def _():
        to = me + quarter
        pl.semaphore_signal(barrier, inc=1, device_id={"seq": to, "chan": lead}, device_id_type=MESH)

    for c in loads[2:13]:
        c.start()

    def remote(src, dst, send, recv, to):
        c = pltpu.make_async_remote_copy(
            src_ref=src, dst_ref=dst, send_sem=send, recv_sem=recv, device_id=to, device_id_type=MESH
        )
        c.start()
        return c

    def drain(block, sem):
        pltpu.make_async_copy(block, block, sem).wait()

    def peers(ref, g):
        return ref.at[pl.ds(0, half - 1), pl.ds(groups[g][0], groups[g][1]), :]

    def lines(ref, who, g):
        first, count = groups[g]
        return ref.at[pl.ds(pl.multiple_of(who * chans + first, 8), count), :]

    def weight(who, w_ref):
        return split(w_ref[pl.ds(pl.multiple_of(who * depth, 8), depth), :])

    def project(who, w_ref):
        return dot3(split(tok[who]), weight(who, w_ref))

    @pl.when(mine != lead)
    def _():
        pl.semaphore_wait(barrier, 1)
        pl.semaphore_signal(up_sem, inc=1, device_id={"chan": lead}, device_id_type=MESH)

    @pl.when(mine == lead)
    def _():
        pl.semaphore_wait(up_sem, 1)

    for i, piece in enumerate(pieces):
        loads[13 * i].wait()
        part_of = tok.at[mine, :, piece]
        remote(part_of, part_of, tok_send, tok_recv.at[i], {"chan": 1 - mine})
    loads[1].wait()
    value_sum = project(mine, value_w)
    ahead = weight(1 - mine, value_w)
    for i, piece in enumerate(pieces):
        drain(tok.at[mine, :, piece], tok_recv.at[i])
        there = slice(i * (depth // 2), (i + 1) * (depth // 2))
        value_sum = value_sum + dot3(split(tok[1 - mine, :, there]), tuple(w[there] for w in ahead))
    sent[...] = silu(value_sum).T

    near = sorted(range(half), key=lambda i: (bin(i % max(1, half // 2)).count("1"), i))

    def tell(sem, **who):
        pl.semaphore_signal(sem, inc=1, device_id=who, device_id_type=MESH)

    def cross_values(some):
        for g, (first, count) in enumerate(groups):
            for i in sorted(range(quarter), key=lambda i: bin(i).count("1")):
                to = some + flipped(lax.rem(idx, quarter), i, quarter)
                there = got_x.at[idx, pl.ds(first, count), :]
                remote(lines(sent, to, g), there, x_send, x_recv.at[g], {"seq": half + to})

    @pl.when(jnp.logical_and(by_value, jnp.logical_not(jnp.logical_or(second_z, third_z))))
    def _():
        pl.semaphore_wait(barrier, m * (half - 1))
        tell(all_sem, chan=1 - lead)

        @pl.when(lower)
        def _():
            tell(all_sem, seq=me + quarter, chan=1 - lead)

    @pl.when(jnp.logical_and(by_value, third_z))
    def _():
        pl.semaphore_wait(barrier, m * half)
        tell(all_sem, chan=1 - lead)
        tell(far_sem, seq=me - quarter)

    @pl.when(jnp.logical_and(by_value, second_z))
    def _():
        pl.semaphore_wait(barrier, m * (half - 1 + quarter))
        tell(near_sem, seq=me - quarter)
        cross_values(0)
        pl.semaphore_wait(far_sem, 1)
        tell(far_sem, chan=1 - lead)
        tell(far_sem, seq=me - quarter)
        cross_values(quarter)

    @pl.when(by_result)
    def _():
        pl.semaphore_wait(all_sem, 1)

    for g, (first, count) in enumerate(groups):
        for i in range(half - 1, 0, -1):
            to = flipped(idx, i, half)
            there = got.at[idx, pl.ds(first, count), :]
            remote(lines(sent, to, g), there, a_send, a_recv.at[g], {"seq": side * half + to})
        got[idx, first : first + count, :] = lines(sent, idx, g)[...]

    @pl.when(jnp.logical_and(by_value, first_z))
    def _():
        pl.semaphore_wait(near_sem, 1)
        cross_values(0)
        pl.semaphore_wait(far_sem, 1)
        tell(far_sem, chan=1 - lead)
        cross_values(quarter)

    for c in loads[3:5] + loads[6:13]:
        c.wait()
    low, high = position_blocks(
        n * rows, rows, [(0, half), (half, n)], idx * chans, chans, wave, w_in, b_in, w_mid, b_mid, w_out, decay
    )
    kern, k_cross = [], []
    for first, count in groups:
        own = forward([b[first : first + count] for b in low], turn, mat)
        far = forward([b[first : first + count] for b in high], turn, mat)
        kern.append(own)
        k_cross.append(jnp.concatenate([far[:, :rows] - own[:, rows:], far[:, rows:] + own[:, :rows]], axis=1))

    def part(ref, g):
        first, count = groups[g]
        return [ref[s, first : first + count, :] for s in range(half)]

    for g, (first, count) in enumerate(groups):
        drain(peers(got, g), a_recv.at[g])
        spec = forward(part(got, g), turn, mat)
        spec_ref[g] = spec
        prod_ref[g] = cmul(spec, kern[g])

        @pl.when(jnp.logical_and(side == 1, by_value))
        def _():
            drain(got_x.at[:, pl.ds(first, count), :], x_recv.at[g])
            prod_ref[g] = prod_ref[g] + cmul(forward(part(got_x, g), turn, mat), k_cross[g])

        for s, y in enumerate(backward(prod_ref[g], half, turn, mat)):
            own_out[s, first : first + count, :] = y
        for i in range(half - 1, 0, -1):
            to = flipped(idx, i, half)
            here, there = own_out.at[to, pl.ds(first, count), :], own_in.at[idx, pl.ds(first, count), :]
            remote(here, there, b_send, b_recv.at[g], {"seq": side * half + to})
        own_in[idx, first : first + count, :] = own_out[idx, first : first + count, :]

        @pl.when(jnp.logical_and(lower, by_result))
        def _():
            for s, y in enumerate(backward(cmul(spec_ref[g], k_cross[g]), half, turn, mat)):
                cross_out[s, first : first + count, :] = y
            if g == 0:
                pl.semaphore_wait(far_sem, 1)
            for i in reversed(near):
                to = flipped(idx, i, half)
                here, there = cross_out.at[to, pl.ds(first, count), :], cross_in.at[idx, pl.ds(first, count), :]
                remote(here, there, y_send, y_recv.at[g], {"seq": half + to})

    loads[2].wait()
    gate_sum = project(mine, gate_w)
    for i in range(1, m):
        gate_sum = gate_sum + project(lax.rem(mine + m - i, m), gate_w)
    gate_lines = silu(gate_sum).T.reshape(half, chans, rows)
    loads[5].wait()
    for g, (first, count) in enumerate(groups):
        some = out_w[...].reshape(half, chans, m * depth)[:, first : first + count, :]
        w_high[g], w_low[g] = split(some.reshape(half * count, m * depth))
    other = lax.rem(mine + 1, m)

    def partial(mixed, g, start, size):
        cols = pl.ds(pl.multiple_of(start, 128), size)
        return dot3(mixed, (w_high[g, :, cols], w_low[g, :, cols]))

    sums = [0.0, 0.0]
    for g, (first, count) in enumerate(groups):
        drain(peers(own_in, g), b_recv.at[g])

        @pl.when(jnp.logical_and(side == 1, by_result))
        def _():
            drain(cross_in.at[:, pl.ds(first, count), :], y_recv.at[g])
            own_in[:, first : first + count, :] = (
                own_in[:, first : first + count, :] + cross_in[:, first : first + count, :]
            )

        some = slice(first, first + count)
        mixed = split((gate_lines[:, some, :] * own_in[:, some, :]).reshape(half * count, rows).T)
        if g < len(groups) - 1:
            sums = [t + partial(mixed, g, who * depth, depth) for t, who in zip(sums, (mine, other))]

    part_out[...] = sums[1] + partial(mixed, len(groups) - 1, other * depth, depth)
    remote(part_out, part_in, p_send, p_recv, {"chan": other})
    total = sums[0] + partial(mixed, len(groups) - 1, mine * depth, depth)
    drain(part_in, p_recv)
    result[...] = total + part_in[...]
    for g in range(len(groups)):
        drain(peers(got, g), a_send)
        drain(peers(own_in, g), b_send)

    @pl.when(jnp.logical_and(lower, by_value))
    def _():
        drain(got_x, x_send)

    @pl.when(jnp.logical_and(lower, by_result))
    def _():
        drain(cross_out, y_send)

    drain(tok.at[mine], tok_send)
    drain(part_out, p_send)


def scoped_body(*args):
    pl.run_scoped(
        functools.partial(body, *args), pltpu.SemaphoreType.DMA((14,)), pltpu.SemaphoreType.DMA((6,))
    )


def on_device(
    tokens, gate_weight, value_weight, output_weight, wave_numbers,
    position_in, bias_in, position_mid, bias_mid, position_out, decay_rate,
):
    n, m = lax.axis_size("seq"), lax.axis_size("chan")
    rows, depth = tokens.shape
    width = gate_weight.shape[1]
    half = n // 2
    chans = width // half
    count = chans // 2 if chans % 16 == 0 else chans
    groups = [(first, count) for first in range(0, chans, count)]
    assert m == 2 and n % 4 == 0
    turns, mats = tables(half, rows)
    hbm = pl.BlockSpec(memory_space=pl.ANY)
    vmem = pl.BlockSpec(memory_space=pltpu.VMEM)
    dma = pltpu.SemaphoreType.DMA
    return pl.pallas_call(
        functools.partial(scoped_body, n, m, groups),
        out_shape=pltpu.VMEM((rows, depth), F32),
        in_specs=[hbm] * 13,
        out_specs=vmem,
        scratch_shapes=[
            pltpu.VMEM((1, wave_numbers.shape[0]), jnp.int32),
            pltpu.VMEM(position_in.shape, F32),
            pltpu.VMEM((1, bias_in.shape[0]), F32),
            pltpu.VMEM(position_mid.shape, F32),
            pltpu.VMEM((1, bias_mid.shape[0]), F32),
            pltpu.VMEM(position_out.shape, F32),
            pltpu.VMEM((1, width), F32),
            pltpu.VMEM((m, rows, depth), F32),
            pltpu.VMEM(gate_weight.shape, F32),
            pltpu.VMEM(value_weight.shape, F32),
            pltpu.VMEM(output_weight.shape, F32),
            pltpu.VMEM(turns.shape, F32),
            pltpu.VMEM(mats.shape, BF16),
            pltpu.VMEM((width, rows), F32),
            pltpu.VMEM((half, chans, rows), F32),
            pltpu.VMEM((half, chans, rows), F32),
            pltpu.VMEM((half, chans, rows), F32),
            pltpu.VMEM((half, chans, rows), F32),
            pltpu.VMEM((half, chans, rows), F32),
            pltpu.VMEM((half, chans, rows), F32),
            pltpu.VMEM((len(groups), half * count, 2 * rows), F32),
            pltpu.VMEM((len(groups), half * count, 2 * rows), F32),
            pltpu.VMEM((len(groups), half * count, m * depth), BF16),
            pltpu.VMEM((len(groups), half * count, m * depth), BF16),
            pltpu.VMEM((rows, depth), F32),
            pltpu.VMEM((rows, depth), F32),
            pltpu.SemaphoreType.REGULAR,
            pltpu.SemaphoreType.REGULAR,
            pltpu.SemaphoreType.REGULAR,
            pltpu.SemaphoreType.REGULAR,
            dma((2,)),
            dma((len(groups),)), dma((len(groups),)), dma((len(groups),)), dma((len(groups),)),
            dma,
        ],
        compiler_params=pltpu.CompilerParams(collective_id=0, has_side_effects=True),
    )(
        tokens, gate_weight, value_weight, output_weight, jnp.asarray(turns), jnp.asarray(mats),
        wave_numbers[None, :], position_in, bias_in[None, :], position_mid, bias_mid[None, :],
        position_out, decay_rate[None, :],
    )


def solution(mesh):
    placed = (
        P("seq", "chan"), P(None, "chan"), P(None, "chan"), P("chan", None),
        P(), P(), P(), P(), P(), P(None, "chan"), P("chan"),
    )
    return jax.shard_map(
        on_device, mesh=mesh, in_specs=placed, out_specs=P("seq", "chan"), check_vma=False
    )
```

```python
import functools
import math

import jax
import jax.numpy as jnp
import numpy as np
from jax import lax
from jax.experimental import pallas as pl
from jax.experimental.pallas import tpu as pltpu
from jax.sharding import PartitionSpec as P

PERIOD = 4096
F32 = jnp.float32
BF16 = jnp.bfloat16
MESH = pl.DeviceIdType.MESH


def split(a):
    hi = a.astype(BF16)
    return hi, (a - hi.astype(F32)).astype(BF16)


def mm(a, b, dims=((1,), (0,))):
    return lax.dot_general(a, b, (dims, ((), ())), preferred_element_type=F32)


def dot3(a, b, dims=((1,), (0,))):
    (ah, al), (bh, bl) = a, b
    return mm(ah, bh, dims) + (mm(ah, bl, dims) + mm(al, bh, dims))


def silu(v):
    return v / (1.0 + jnp.exp(-v))


def cmul_const(z, angle):
    c, s = math.cos(angle), math.sin(angle)
    re, im = z
    if abs(s) < 1e-12:
        return (re, im) if c > 0 else (-re, -im)
    if abs(c) < 1e-12:
        return (-im, re) if s > 0 else (im, -re)
    return (re * c - im * s, re * s + im * c)


def fft(xs, sign):
    n = len(xs)
    if n == 1:
        return xs
    even, odd = fft(xs[0::2], sign), fft(xs[1::2], sign)
    low, high = [], []
    for k in range(n // 2):
        er, ei = even[k]
        tr, ti = cmul_const(odd[k], sign * 2.0 * math.pi * k / n)
        low.append((er + tr, ei + ti))
        high.append((er - tr, ei - ti))
    return low + high


def tables(outer, inner):
    length = outer * inner
    r = np.arange(inner)
    turn = 2.0 * np.pi * np.outer(np.arange(outer) + 0.25, r) / length
    turns = np.concatenate([np.cos(turn), np.sin(turn)], 0).astype(np.float32)
    ang = 2.0 * np.pi * (np.outer(r, r) % inner) / inner
    c, s = np.cos(ang), np.sin(ang)
    fwd = np.block([[c, -s], [s, c]]).astype(np.float32)
    inv = (np.block([[c, s], [-s, c]]) / length).astype(np.float32)

    def halves(a):
        hi = a.astype(jnp.bfloat16)
        return [hi, (a - hi.astype(np.float32)).astype(jnp.bfloat16)]

    return turns, np.stack(halves(fwd) + halves(inv))


def column(row, first, count):
    n = row.shape[1]
    i = lax.broadcasted_iota(jnp.int32, (count, n), 0)
    j = lax.broadcasted_iota(jnp.int32, (count, n), 1)
    picked = jnp.where(j == i + first, jnp.broadcast_to(row, (count, n)), jnp.zeros_like(row))
    return jnp.sum(picked, axis=1, keepdims=True)


def forward(blocks, turn_ref, mat_ref):
    outer = len(blocks)
    step = -2.0 * math.pi / (4 * outer)
    twisted = [(b * math.cos(step * s), b * math.sin(step * s)) if s else (b, None) for s, b in enumerate(blocks)]
    twisted[0] = (blocks[0], jnp.zeros_like(blocks[0]))
    rows = []
    for k, (re, im) in enumerate(fft(twisted, -1.0)):
        c, s = turn_ref[k : k + 1, :], turn_ref[outer + k : outer + k + 1, :]
        rows.append(jnp.concatenate([re * c + im * s, im * c - re * s], axis=1))
    grid = jnp.concatenate(rows, axis=0)
    return dot3(split(grid), (mat_ref[0], mat_ref[1]))


def backward(spectrum, outer, turn_ref, mat_ref):
    back = dot3(split(spectrum), (mat_ref[2], mat_ref[3]))
    chans, inner = spectrum.shape[0] // outer, spectrum.shape[1] // 2
    zs = []
    for k in range(outer):
        re = back[k * chans : (k + 1) * chans, :inner]
        im = back[k * chans : (k + 1) * chans, inner:]
        c, s = turn_ref[k : k + 1, :], turn_ref[outer + k : outer + k + 1, :]
        zs.append((re * c - im * s, re * s + im * c))
    ys = fft(zs, 1.0)
    step = 2.0 * math.pi / (4 * outer)
    return [re * math.cos(step * s) - im * math.sin(step * s) for s, (re, im) in enumerate(ys)]


def cmul(a, b):
    half = a.shape[1] // 2
    ar, ai, br, bi = a[:, :half], a[:, half:], b[:, :half], b[:, half:]
    return jnp.concatenate([ar * br - ai * bi, ar * bi + ai * br], axis=1)


def position_blocks(length, inner, parts, first, chans, wave, w_in, b_in, w_mid, b_mid, w_out, decay):
    waves = wave.shape[1]
    hid = w_in.shape[1]
    wcol = column(wave[...], 0, waves)
    unit = 2.0 * math.pi / PERIOD

    def trig(spots):
        ang = (lax.rem(spots * wcol, PERIOD)).astype(F32) * unit
        return jnp.cos(ang), jnp.sin(ang)

    rc, rs = trig(lax.broadcasted_iota(jnp.int32, (waves, inner), 1))
    sc, ss = trig(lax.broadcasted_iota(jnp.int32, (waves, max(length // inner, 128)), 1) * inner)
    bi, bm = column(b_in[...], 0, hid), column(b_mid[...], 0, w_mid.shape[1])
    wi, wm = split(w_in[...].T), split(w_mid[...].T)
    width = w_out.shape[1]
    oh, ol = split(w_out[...])
    nt = ((1,), (1,))
    i = lax.broadcasted_iota(jnp.int32, (chans, width), 0)
    j = lax.broadcasted_iota(jnp.int32, (chans, width), 1)
    pick = jnp.where(j == i + first, 1.0, 0.0).astype(BF16)
    own = (mm(pick, oh, nt).astype(BF16), mm(pick, ol, nt).astype(BF16))
    dec = column(decay[...], first, chans)
    gain = jnp.sqrt(2.0 * dec / length)
    most = max(1, 2048 // inner)
    result = []
    for start, stop in parts:
        blocks = []
        for s0 in range(start, stop, most):
            some = range(s0, min(stop, s0 + most))
            cs, sn = [], []
            for s in some:
                a, b = sc[:, s : s + 1], ss[:, s : s + 1]
                cs.append(rc * a - rs * b)
                sn.append(rs * a + rc * b)
            feats = jnp.concatenate([jnp.concatenate(cs, 1), jnp.concatenate(sn, 1)], 0)
            h = jnp.maximum(dot3(wi, split(feats)) + bi, 0.0)
            h = jnp.maximum(dot3(wm, split(h)) + bm, 0.0)
            shape = dot3(own, split(h))
            n = (lax.broadcasted_iota(jnp.int32, shape.shape, 1) + s0 * inner).astype(F32) / length
            kern = shape * (jnp.exp(-dec * n) * gain)
            blocks += [kern[:, q * inner : (q + 1) * inner] for q in range(len(some))]
        result.append(blocks)
    return result


def body(
    n, m, groups,
    tok_hbm, gate_hbm, value_hbm, out_hbm, turn_hbm, mat_hbm,
    wave_hbm, w_in_hbm, b_in_hbm, w_mid_hbm, b_mid_hbm, w_out_hbm, decay_hbm,
    result,
    wave, w_in, b_in, w_mid, b_mid, w_out, decay,
    tok, gate_w, value_w, out_w, turn, mat,
    sent, got, got_x, own_out, own_in, cross_out, cross_in, spec_ref, prod_ref, w_high, w_low, part_out, part_in,
    up_sem, all_sem, near_sem, far_sem, tok_recv, a_recv, x_recv, b_recv, y_recv, p_recv, load_sem, send_sems,
):
    tok_send, a_send, x_send, b_send, y_send, p_send = (send_sems.at[i] for i in range(6))
    me, mine = lax.axis_index("seq"), lax.axis_index("chan")
    rows, depth = tok_hbm.shape
    width = value_w.shape[1]
    half = n // 2
    side, idx = me // half, lax.rem(me, half)
    chans = width // half

    def flipped(at, i, count):
        if count & (count - 1):
            return lax.rem(at + i, count)
        bit, to = 1, 0
        while bit < count:
            here = lax.rem(at // bit, 2)
            to = to + (1 - here if i & bit else here) * bit
            bit *= 2
        return to

    pieces = [pl.ds(first, depth // 2) for first in (0, depth // 2)]
    loads = [
        pltpu.make_async_copy(src, dst, load_sem.at[i])
        for i, (src, dst) in enumerate(
            [
                (tok_hbm.at[:, pieces[0]], tok.at[mine, :, pieces[0]]), (value_hbm, value_w), (gate_hbm, gate_w), (mat_hbm, mat), (turn_hbm, turn), (out_hbm, out_w),
                (wave_hbm, wave), (w_in_hbm, w_in), (b_in_hbm, b_in), (w_mid_hbm, w_mid), (b_mid_hbm, b_mid), (w_out_hbm, w_out), (decay_hbm, decay),
                (tok_hbm.at[:, pieces[1]], tok.at[mine, :, pieces[1]]),
            ]
        )
    ]
    for c in (loads[0], loads[13], loads[1]):
        c.start()

    barrier = pltpu.get_barrier_semaphore()
    lead, quarter = m - 1, half // 2
    lower, by_value = side == 0, mine == lead
    first_z, second_z = jnp.logical_and(lower, idx < quarter), jnp.logical_and(lower, idx >= quarter)
    third_z = jnp.logical_and(side == 1, idx < quarter)
    by_result = jnp.logical_not(by_value)
    @pl.when(mine == lead)
    def _():
        pl.semaphore_signal(barrier, inc=1, device_id={"chan": 1 - lead}, device_id_type=MESH)

    for i in range(half - 1, 0, -1):
        to = side * half + flipped(idx, i, half)
        pl.semaphore_signal(barrier, inc=1, device_id={"seq": to, "chan": lead}, device_id_type=MESH)

    @pl.when(third_z)
    def _():
        for to in range(quarter, half):
            pl.semaphore_signal(barrier, inc=1, device_id={"seq": to, "chan": lead}, device_id_type=MESH)

    @pl.when(second_z)
    def _():
        to = me + quarter
        pl.semaphore_signal(barrier, inc=1, device_id={"seq": to, "chan": lead}, device_id_type=MESH)

    for c in loads[2:13]:
        c.start()

    def remote(src, dst, send, recv, to):
        c = pltpu.make_async_remote_copy(
            src_ref=src, dst_ref=dst, send_sem=send, recv_sem=recv, device_id=to, device_id_type=MESH
        )
        c.start()
        return c

    def drain(block, sem):
        pltpu.make_async_copy(block, block, sem).wait()

    def peers(ref, g):
        return ref.at[pl.ds(0, half - 1), pl.ds(groups[g][0], groups[g][1]), :]

    def lines(ref, who, g):
        first, count = groups[g]
        return ref.at[pl.ds(pl.multiple_of(who * chans + first, 8), count), :]

    def weight(who, w_ref):
        return split(w_ref[pl.ds(pl.multiple_of(who * depth, 8), depth), :])

    def project(who, w_ref):
        return dot3(split(tok[who]), weight(who, w_ref))

    @pl.when(mine != lead)
    def _():
        pl.semaphore_wait(barrier, 1)
        pl.semaphore_signal(up_sem, inc=1, device_id={"chan": lead}, device_id_type=MESH)

    @pl.when(mine == lead)
    def _():
        pl.semaphore_wait(up_sem, 1)

    for i, piece in enumerate(pieces):
        loads[13 * i].wait()
        part_of = tok.at[mine, :, piece]
        remote(part_of, part_of, tok_send, tok_recv.at[i], {"chan": 1 - mine})
    loads[1].wait()
    value_sum = project(mine, value_w)
    ahead = weight(1 - mine, value_w)
    for i, piece in enumerate(pieces):
        drain(tok.at[mine, :, piece], tok_recv.at[i])
        there = slice(i * (depth // 2), (i + 1) * (depth // 2))
        value_sum = value_sum + dot3(split(tok[1 - mine, :, there]), tuple(w[there] for w in ahead))
    sent[...] = silu(value_sum).T

    near = sorted(range(half), key=lambda i: (bin(i % max(1, half // 2)).count("1"), i))

    def tell(sem, **who):
        pl.semaphore_signal(sem, inc=1, device_id=who, device_id_type=MESH)

    def cross_values(some):
        for g, (first, count) in enumerate(groups):
            for i in sorted(range(quarter), key=lambda i: -bin(i).count("1")):
                to = some + flipped(lax.rem(idx, quarter), i, quarter)
                there = got_x.at[idx, pl.ds(first, count), :]
                remote(lines(sent, to, g), there, x_send, x_recv.at[g], {"seq": half + to})

    @pl.when(jnp.logical_and(by_value, jnp.logical_not(jnp.logical_or(second_z, third_z))))
    def _():
        pl.semaphore_wait(barrier, m * (half - 1))
        tell(all_sem, chan=1 - lead)

        @pl.when(lower)
        def _():
            tell(all_sem, seq=me + quarter, chan=1 - lead)

    @pl.when(jnp.logical_and(by_value, third_z))
    def _():
        pl.semaphore_wait(barrier, m * half)
        tell(all_sem, chan=1 - lead)
        tell(far_sem, seq=me - quarter)

    @pl.when(jnp.logical_and(by_value, second_z))
    def _():
        pl.semaphore_wait(barrier, m * (half - 1 + quarter))
        tell(near_sem, seq=me - quarter)
        cross_values(0)

    @pl.when(by_result)
    def _():
        pl.semaphore_wait(all_sem, 1)

    for g, (first, count) in enumerate(groups):
        for i in range(half - 1, 0, -1):
            to = flipped(idx, i, half)
            there = got.at[idx, pl.ds(first, count), :]
            remote(lines(sent, to, g), there, a_send, a_recv.at[g], {"seq": side * half + to})
        got[idx, first : first + count, :] = lines(sent, idx, g)[...]

    @pl.when(jnp.logical_and(by_value, second_z))
    def _():
        pl.semaphore_wait(far_sem, 1)
        tell(far_sem, chan=1 - lead)
        tell(far_sem, seq=me - quarter)
        cross_values(quarter)

    @pl.when(jnp.logical_and(by_value, first_z))
    def _():
        pl.semaphore_wait(near_sem, 1)
        cross_values(0)
        pl.semaphore_wait(far_sem, 1)
        tell(far_sem, chan=1 - lead)
        cross_values(quarter)

    for c in loads[3:5] + loads[6:13]:
        c.wait()
    low, high = position_blocks(
        n * rows, rows, [(0, half), (half, n)], idx * chans, chans, wave, w_in, b_in, w_mid, b_mid, w_out, decay
    )
    kern, k_cross = [], []
    for first, count in groups:
        own = forward([b[first : first + count] for b in low], turn, mat)
        far = forward([b[first : first + count] for b in high], turn, mat)
        kern.append(own)
        k_cross.append(jnp.concatenate([far[:, :rows] - own[:, rows:], far[:, rows:] + own[:, :rows]], axis=1))

    def part(ref, g):
        first, count = groups[g]
        return [ref[s, first : first + count, :] for s in range(half)]

    for g, (first, count) in enumerate(groups):
        drain(peers(got, g), a_recv.at[g])
        spec = forward(part(got, g), turn, mat)
        spec_ref[g] = spec
        prod_ref[g] = cmul(spec, kern[g])

        @pl.when(jnp.logical_and(side == 1, by_value))
        def _():
            drain(got_x.at[:, pl.ds(first, count), :], x_recv.at[g])
            prod_ref[g] = prod_ref[g] + cmul(forward(part(got_x, g), turn, mat), k_cross[g])

        for s, y in enumerate(backward(prod_ref[g], half, turn, mat)):
            own_out[s, first : first + count, :] = y
        for i in range(half - 1, 0, -1):
            to = flipped(idx, i, half)
            here, there = own_out.at[to, pl.ds(first, count), :], own_in.at[idx, pl.ds(first, count), :]
            remote(here, there, b_send, b_recv.at[g], {"seq": side * half + to})
        own_in[idx, first : first + count, :] = own_out[idx, first : first + count, :]

        @pl.when(jnp.logical_and(lower, by_result))
        def _():
            for s, y in enumerate(backward(cmul(spec_ref[g], k_cross[g]), half, turn, mat)):
                cross_out[s, first : first + count, :] = y
            if g == 0:
                pl.semaphore_wait(far_sem, 1)
            for i in reversed(near):
                to = flipped(idx, i, half)
                here, there = cross_out.at[to, pl.ds(first, count), :], cross_in.at[idx, pl.ds(first, count), :]
                remote(here, there, y_send, y_recv.at[g], {"seq": half + to})

    loads[2].wait()
    gate_sum = project(mine, gate_w)
    for i in range(1, m):
        gate_sum = gate_sum + project(lax.rem(mine + m - i, m), gate_w)
    gate_lines = silu(gate_sum).T.reshape(half, chans, rows)
    loads[5].wait()
    for g, (first, count) in enumerate(groups):
        some = out_w[...].reshape(half, chans, m * depth)[:, first : first + count, :]
        w_high[g], w_low[g] = split(some.reshape(half * count, m * depth))
    other = lax.rem(mine + 1, m)

    def partial(mixed, g, start, size):
        cols = pl.ds(pl.multiple_of(start, 128), size)
        return dot3(mixed, (w_high[g, :, cols], w_low[g, :, cols]))

    sums = [0.0, 0.0]
    for g, (first, count) in enumerate(groups):
        drain(peers(own_in, g), b_recv.at[g])

        @pl.when(jnp.logical_and(side == 1, by_result))
        def _():
            drain(cross_in.at[:, pl.ds(first, count), :], y_recv.at[g])
            own_in[:, first : first + count, :] = (
                own_in[:, first : first + count, :] + cross_in[:, first : first + count, :]
            )

        some = slice(first, first + count)
        mixed = split((gate_lines[:, some, :] * own_in[:, some, :]).reshape(half * count, rows).T)
        if g < len(groups) - 1:
            sums = [t + partial(mixed, g, who * depth, depth) for t, who in zip(sums, (mine, other))]

    part_out[...] = sums[1] + partial(mixed, len(groups) - 1, other * depth, depth)
    remote(part_out, part_in, p_send, p_recv, {"chan": other})
    total = sums[0] + partial(mixed, len(groups) - 1, mine * depth, depth)
    drain(part_in, p_recv)
    result[...] = total + part_in[...]
    for g in range(len(groups)):
        drain(peers(got, g), a_send)
        drain(peers(own_in, g), b_send)

    @pl.when(jnp.logical_and(lower, by_value))
    def _():
        drain(got_x, x_send)

    @pl.when(jnp.logical_and(lower, by_result))
    def _():
        drain(cross_out, y_send)

    drain(tok.at[mine], tok_send)
    drain(part_out, p_send)


def scoped_body(*args):
    pl.run_scoped(
        functools.partial(body, *args), pltpu.SemaphoreType.DMA((14,)), pltpu.SemaphoreType.DMA((6,))
    )


def on_device(
    tokens, gate_weight, value_weight, output_weight, wave_numbers,
    position_in, bias_in, position_mid, bias_mid, position_out, decay_rate,
):
    n, m = lax.axis_size("seq"), lax.axis_size("chan")
    rows, depth = tokens.shape
    width = gate_weight.shape[1]
    half = n // 2
    chans = width // half
    count = chans // 2 if chans % 16 == 0 else chans
    groups = [(first, count) for first in range(0, chans, count)]
    assert m == 2 and n % 4 == 0
    turns, mats = tables(half, rows)
    hbm = pl.BlockSpec(memory_space=pl.ANY)
    vmem = pl.BlockSpec(memory_space=pltpu.VMEM)
    dma = pltpu.SemaphoreType.DMA
    return pl.pallas_call(
        functools.partial(scoped_body, n, m, groups),
        out_shape=pltpu.VMEM((rows, depth), F32),
        in_specs=[hbm] * 13,
        out_specs=vmem,
        scratch_shapes=[
            pltpu.VMEM((1, wave_numbers.shape[0]), jnp.int32),
            pltpu.VMEM(position_in.shape, F32),
            pltpu.VMEM((1, bias_in.shape[0]), F32),
            pltpu.VMEM(position_mid.shape, F32),
            pltpu.VMEM((1, bias_mid.shape[0]), F32),
            pltpu.VMEM(position_out.shape, F32),
            pltpu.VMEM((1, width), F32),
            pltpu.VMEM((m, rows, depth), F32),
            pltpu.VMEM(gate_weight.shape, F32),
            pltpu.VMEM(value_weight.shape, F32),
            pltpu.VMEM(output_weight.shape, F32),
            pltpu.VMEM(turns.shape, F32),
            pltpu.VMEM(mats.shape, BF16),
            pltpu.VMEM((width, rows), F32),
            pltpu.VMEM((half, chans, rows), F32),
            pltpu.VMEM((half, chans, rows), F32),
            pltpu.VMEM((half, chans, rows), F32),
            pltpu.VMEM((half, chans, rows), F32),
            pltpu.VMEM((half, chans, rows), F32),
            pltpu.VMEM((half, chans, rows), F32),
            pltpu.VMEM((len(groups), half * count, 2 * rows), F32),
            pltpu.VMEM((len(groups), half * count, 2 * rows), F32),
            pltpu.VMEM((len(groups), half * count, m * depth), BF16),
            pltpu.VMEM((len(groups), half * count, m * depth), BF16),
            pltpu.VMEM((rows, depth), F32),
            pltpu.VMEM((rows, depth), F32),
            pltpu.SemaphoreType.REGULAR,
            pltpu.SemaphoreType.REGULAR,
            pltpu.SemaphoreType.REGULAR,
            pltpu.SemaphoreType.REGULAR,
            dma((2,)),
            dma((len(groups),)), dma((len(groups),)), dma((len(groups),)), dma((len(groups),)),
            dma,
        ],
        compiler_params=pltpu.CompilerParams(collective_id=0, has_side_effects=True),
    )(
        tokens, gate_weight, value_weight, output_weight, jnp.asarray(turns), jnp.asarray(mats),
        wave_numbers[None, :], position_in, bias_in[None, :], position_mid, bias_mid[None, :],
        position_out, decay_rate[None, :],
    )


def solution(mesh):
    placed = (
        P("seq", "chan"), P(None, "chan"), P(None, "chan"), P("chan", None),
        P(), P(), P(), P(), P(), P(None, "chan"), P("chan"),
    )
    return jax.shard_map(
        on_device, mesh=mesh, in_specs=placed, out_specs=P("seq", "chan"), check_vma=False
    )
```
